8 devices in a mesh: fsdp: 8 (over z, y, x, core).
Axes of the slice: x: 2, y: 2, z: 1, core: 2. Of those that a mesh axis runs over, the one named last changes fastest.
Arguments:
- x_resid: bfloat16 [32, 1024, 1024], P('fsdp')
- g_mlp: float32 [1024], P('fsdp')
- w_gate: bfloat16 [1024, 2816], P('fsdp')
- w_up: bfloat16 [1024, 2816], P('fsdp')
- w_down: bfloat16 [2816, 1024], P('fsdp')
- g_attn: float32 [1024], P('fsdp')
- w_dq: bfloat16 [1024, 384], P('fsdp')
- g_q: float32 [384], P('fsdp')
- w_uq: bfloat16 [384, 1536], P('fsdp')
- w_dkv: bfloat16 [1024, 320], P('fsdp')
- g_kv: float32 [256], P('fsdp')
- w_uk: bfloat16 [256, 1024], P('fsdp')
- w_uv: bfloat16 [256, 1024], P('fsdp')
- w_out: bfloat16 [1024, 1024], P('fsdp')
- g_moe: float32 [1024], P('fsdp')
- w_router: float32 [64, 1024], replicated
- we_gate: bfloat16 [64, 1024, 256], P('fsdp')
- we_up: bfloat16 [64, 1024, 256], P('fsdp')
- we_down: bfloat16 [64, 256, 1024], P('fsdp')
- ws_gate: bfloat16 [1024, 256], replicated
- ws_up: bfloat16 [1024, 256], replicated
- ws_down: bfloat16 [256, 1024], replicated
- expert_ids: int32 [32, 1024, 8], P('fsdp')
Outputs:
- output: bfloat16 [32, 1024, 1024], P('fsdp')
All inputs are finite; a program needn't handle non-finite values.
Results may differ from the reference program's by a relative error of at most 0.0192166.
Values are sent between devices in bfloat16 or wider.
A program may use at most 1 GiB of HBM per device.

```python
import jax
import jax.numpy as jnp
from jax import lax

D = 1024
FF = 2816
HEADS = 8
Q_RANK = 384
KV_RANK = 256
NOPE = 128
ROPE = 64
VHEAD = 128
EXPERTS = 64
INTER = 256
TOP = 8
SHARED = 1
SEQ = 1024
SEQS_DEV = 4
GROUP = 8
ROPE_BASE = 10000
EPS = 1e-6
ROUTE_SCALE = 2.5
NSEQS = GROUP * SEQS_DEV
TOK_DEV = SEQS_DEV * SEQ
TOKENS = NSEQS * SEQ
CAP = 2 * TOK_DEV * TOP // EXPERTS
QK_SCALE = (NOPE + ROPE) ** -0.5


def draw_routes(key):
    half = EXPERTS // 2
    mean_load = TOK_DEV * TOP // EXPERTS
    slot_ids = jnp.arange(TOK_DEV * TOP)

    def one_block(block_key):
        key_a, key_b, key_c = jax.random.split(block_key, 3)
        shift = jax.random.randint(key_a, (half,), -mean_load, mean_load + 1)
        shift = jnp.where(jnp.arange(half) == 0, mean_load, shift)
        counts = jnp.stack([mean_load + shift, mean_load - shift], axis=1).reshape(EXPERTS)
        ends = jnp.cumsum(counts)
        sorted_ids = jnp.sum((ends[None, :] <= slot_ids[:, None]).astype(jnp.int32), axis=1)
        relabel = jax.random.permutation(key_b, EXPERTS)
        grid = relabel[sorted_ids].reshape(TOP, TOK_DEV).T
        shuffle = jax.random.permutation(key_c, TOK_DEV)
        return grid[shuffle]

    blocks = lax.map(one_block, jax.random.split(key, GROUP))
    return blocks.reshape(NSEQS, SEQ, TOP).astype(jnp.int32)


def normal_draw(key, shape, scale):
    return (jax.random.normal(key, shape, jnp.float32) * scale).astype(jnp.bfloat16)


def gain_draw(key, size):
    return 1.0 + 0.4 * jax.random.normal(key, (size,), jnp.float32)


def setup_inputs(seed: int = 0) -> dict:
    keys = jax.random.split(jax.random.key(seed), 23)
    inner = SHARED * INTER
    return {
        "x_resid": jax.random.normal(keys[0], (NSEQS, SEQ, D), jnp.float32).astype(jnp.bfloat16),
        "g_mlp": gain_draw(keys[1], D),
        "w_gate": normal_draw(keys[2], (D, FF), D ** -0.5),
        "w_up": normal_draw(keys[3], (D, FF), D ** -0.5),
        "w_down": normal_draw(keys[4], (FF, D), FF ** -0.5),
        "g_attn": gain_draw(keys[5], D),
        "w_dq": normal_draw(keys[6], (D, Q_RANK), D ** -0.5),
        "g_q": gain_draw(keys[7], Q_RANK),
        "w_uq": normal_draw(keys[8], (Q_RANK, HEADS * (NOPE + ROPE)), Q_RANK ** -0.5),
        "w_dkv": normal_draw(keys[9], (D, KV_RANK + ROPE), D ** -0.5),
        "g_kv": gain_draw(keys[10], KV_RANK),
        "w_uk": normal_draw(keys[11], (KV_RANK, HEADS * NOPE), 2.5 * KV_RANK ** -0.5),
        "w_uv": normal_draw(keys[12], (KV_RANK, HEADS * VHEAD), KV_RANK ** -0.5),
        "w_out": normal_draw(keys[13], (HEADS * VHEAD, D), (HEADS * VHEAD) ** -0.5),
        "g_moe": gain_draw(keys[14], D),
        "w_router": 2.0 * D ** -0.5 * jax.random.normal(keys[15], (EXPERTS, D), jnp.float32),
        "we_gate": normal_draw(keys[16], (EXPERTS, D, INTER), D ** -0.5),
        "we_up": normal_draw(keys[17], (EXPERTS, D, INTER), D ** -0.5),
        "we_down": normal_draw(keys[18], (EXPERTS, INTER, D), INTER ** -0.5),
        "ws_gate": normal_draw(keys[19], (D, inner), D ** -0.5),
        "ws_up": normal_draw(keys[20], (D, inner), D ** -0.5),
        "ws_down": normal_draw(keys[21], (inner, D), inner ** -0.5),
        "expert_ids": draw_routes(keys[22]),
    }


def rms_norm(vals, gain):
    vals = vals.astype(jnp.float32)
    scaled = vals * lax.rsqrt(jnp.mean(vals * vals, axis=-1, keepdims=True) + EPS)
    return (scaled * gain).astype(jnp.bfloat16)


def swiglu(rows, w_gate, w_up, w_down):
    gate = jnp.dot(rows, w_gate, preferred_element_type=jnp.float32)
    upper = jnp.dot(rows, w_up, preferred_element_type=jnp.float32)
    hidden = (jax.nn.silu(gate) * upper).astype(jnp.bfloat16)
    return jnp.dot(hidden, w_down, preferred_element_type=jnp.float32).astype(jnp.bfloat16)


def rotate(vals, cos_t, sin_t):
    half = vals.shape[-1] // 2
    first = vals[..., :half].astype(jnp.float32)
    second = vals[..., half:].astype(jnp.float32)
    return jnp.concatenate([first * cos_t - second * sin_t, second * cos_t + first * sin_t], axis=-1).astype(jnp.bfloat16)


def rope_tables():
    positions = jnp.arange(SEQ).astype(jnp.float32)
    inv_freq = 1.0 / (ROPE_BASE ** (jnp.arange(0, ROPE, 2).astype(jnp.float32) / ROPE))
    angles = positions[:, None] * inv_freq[None, :]
    return jnp.cos(angles), jnp.sin(angles)


def attention(normed, w_dq, g_q, w_uq, w_dkv, g_kv, w_uk, w_uv, w_out):
    cos_t, sin_t = rope_tables()
    q_lat = jnp.dot(normed, w_dq, preferred_element_type=jnp.float32).astype(jnp.bfloat16)
    q_all = jnp.dot(rms_norm(q_lat, g_q), w_uq, preferred_element_type=jnp.float32).astype(jnp.bfloat16)
    q_all = q_all.reshape(NSEQS, SEQ, HEADS, NOPE + ROPE)
    q_nope = q_all[..., :NOPE]
    q_rot = rotate(q_all[..., NOPE:], cos_t[:, None, :], sin_t[:, None, :])
    kv_all = jnp.dot(normed, w_dkv, preferred_element_type=jnp.float32).astype(jnp.bfloat16)
    latent = rms_norm(kv_all[:, :KV_RANK], g_kv)
    k_rot = rotate(kv_all[:, KV_RANK:].reshape(NSEQS, SEQ, ROPE), cos_t, sin_t)
    k_nope = jnp.dot(latent, w_uk, preferred_element_type=jnp.float32).astype(jnp.bfloat16).reshape(NSEQS, SEQ, HEADS, NOPE)
    values = jnp.dot(latent, w_uv, preferred_element_type=jnp.float32).astype(jnp.bfloat16).reshape(NSEQS, SEQ, HEADS, VHEAD)
    causal = jnp.arange(SEQ)[:, None] >= jnp.arange(SEQ)[None, :]

    def one_seq(parts):
        nope_q, rot_q, nope_k, rot_k, seq_vals = parts
        scores = jnp.einsum("qhd,khd->hqk", nope_q.astype(jnp.float32), nope_k.astype(jnp.float32))
        scores = scores + jnp.einsum("qhd,kd->hqk", rot_q.astype(jnp.float32), rot_k.astype(jnp.float32))
        scores = jnp.where(causal[None], scores * QK_SCALE, -jnp.inf)
        attn_probs = jax.nn.softmax(scores, axis=-1).astype(jnp.bfloat16)
        return jnp.einsum("hqk,khd->qhd", attn_probs.astype(jnp.float32), seq_vals.astype(jnp.float32)).astype(jnp.bfloat16)

    attended = lax.map(one_seq, (q_nope, q_rot, k_nope, k_rot, values))
    return jnp.dot(attended.reshape(TOKENS, HEADS * VHEAD), w_out, preferred_element_type=jnp.float32).astype(jnp.bfloat16)


def routed_sum(u_norm, w_router, we_gate, we_up, we_down, expert_ids):
    choice_ids = expert_ids.reshape(TOKENS, TOP)
    logits = jnp.dot(u_norm.astype(jnp.float32), w_router.T)
    picked = jnp.take_along_axis(jax.nn.sigmoid(logits), choice_ids, axis=1)
    gates = (ROUTE_SCALE * picked / jnp.sum(picked, axis=1, keepdims=True)).reshape(TOKENS * TOP)
    flat_ids = choice_ids.reshape(TOKENS * TOP)
    order = jnp.argsort(flat_ids, stable=True)
    counts = jnp.bincount(flat_ids, length=EXPERTS)
    starts = jnp.cumsum(counts) - counts
    window = GROUP * CAP
    padded = jnp.concatenate([order, jnp.zeros((window,), order.dtype)])

    def one_expert(total, expert):
        picks = lax.dynamic_slice(padded, (starts[expert],), (window,))
        valid = jnp.arange(window) < counts[expert]
        rows = picks // TOP
        outputs = swiglu(u_norm[rows], we_gate[expert], we_up[expert], we_down[expert])
        weight = jnp.where(valid, gates[picks], 0.0)
        return total.at[rows].add(outputs.astype(jnp.float32) * weight[:, None]), None

    total, _ = lax.scan(one_expert, jnp.zeros((TOKENS, D), jnp.float32), jnp.arange(EXPERTS))
    return total


def reference(x_resid, g_mlp, w_gate, w_up, w_down, g_attn, w_dq, g_q, w_uq, w_dkv, g_kv, w_uk, w_uv, w_out, g_moe, w_router, we_gate, we_up, we_down, ws_gate, ws_up, ws_down, expert_ids):
    flat_x = x_resid.reshape(TOKENS, D)
    mlp_out = swiglu(rms_norm(flat_x, g_mlp), w_gate, w_up, w_down)
    h_one = (flat_x.astype(jnp.float32) + mlp_out.astype(jnp.float32)).astype(jnp.bfloat16)
    attn_out = attention(rms_norm(h_one, g_attn), w_dq, g_q, w_uq, w_dkv, g_kv, w_uk, w_uv, w_out)
    h_two = (h_one.astype(jnp.float32) + attn_out.astype(jnp.float32)).astype(jnp.bfloat16)
    u_norm = rms_norm(h_two, g_moe)
    shared = swiglu(u_norm, ws_gate, ws_up, ws_down)
    routed = routed_sum(u_norm, w_router, we_gate, we_up, we_down, expert_ids)
    z_out = (h_two.astype(jnp.float32) + shared.astype(jnp.float32) + routed).astype(jnp.bfloat16)
    return z_out.reshape(NSEQS, SEQ, D)
```

```python
import functools

import jax
import jax.numpy as jnp
from jax import lax
from jax.experimental import pallas as pl
from jax.experimental.pallas import tpu as pltpu
from jax.sharding import PartitionSpec as P


AXIS = "fsdp"
ROPE_BASE = 10000.0
EPS = 1e-6
ROUTE_SCALE = 2.5
TILE = 256
PITCH = TILE + 8
LANES = 128
CHUNKS = (2, 2, 2, 2)
VMEM_LIMIT = 60 * 1024 * 1024


def rms_norm(vals, gain):
    vals = vals.astype(jnp.float32)
    scaled = vals * lax.rsqrt(jnp.mean(vals * vals, axis=-1, keepdims=True) + EPS)
    return (scaled * gain).astype(jnp.bfloat16)


def mm(lhs, rhs):
    return jnp.dot(lhs, rhs, preferred_element_type=jnp.float32)


def swiglu(rows, w_gate, w_up, w_down):
    hidden = (jax.nn.silu(mm(rows, w_gate)) * mm(rows, w_up)).astype(jnp.bfloat16)
    return mm(hidden, w_down).astype(jnp.bfloat16)


def to_blocks(shard):
    rows, cols = shard.shape
    return shard.reshape(rows, cols // LANES, LANES).transpose(1, 0, 2).reshape(-1, LANES)


def from_blocks(gathered, start, rows, cols):
    groups = gathered.shape[0]
    blocks = cols // LANES
    part = gathered[:, start : start + rows * blocks].reshape(groups, blocks, rows, LANES)
    return part.transpose(0, 2, 1, 3).reshape(groups * rows, cols)


def attn_kernel(scale, block, qn_ref, qr_ref, kn_ref, kr_ref, v_ref, o_ref):
    seq = qn_ref.shape[0]
    keys = jnp.concatenate([kn_ref[...], kr_ref[...]], axis=1)
    vals = v_ref[...]
    for start in range(0, seq, block):
        stop = start + block
        query = jnp.concatenate([qn_ref[start:stop, :], qr_ref[start:stop, :]], axis=1)
        scores = lax.dot_general(query, keys[:stop], (((1,), (1,)), ((), ())), preferred_element_type=jnp.float32)
        row = lax.broadcasted_iota(jnp.int32, scores.shape, 0) + start
        col = lax.broadcasted_iota(jnp.int32, scores.shape, 1)
        scores = jnp.where(row >= col, scores * scale, -jnp.inf)
        expo = jnp.exp(scores - jnp.max(scores, axis=1, keepdims=True))
        probs = (expo * (1.0 / jnp.sum(expo, axis=1, keepdims=True))).astype(jnp.bfloat16)
        o_ref[start:stop, :] = mm(probs, vals[:stop]).astype(jnp.bfloat16)


def attention_core(q_nope, q_rot, k_nope, k_rot, values, seq_len, scale):
    tokens, width = q_nope.shape
    seqs, heads = tokens // seq_len, width // LANES
    spec = lambda fn: pl.BlockSpec((seq_len, LANES), fn)
    return pl.pallas_call(
        functools.partial(attn_kernel, scale, 256),
        grid=(seqs, heads),
        in_specs=[
            spec(lambda s, h: (s, h)),
            spec(lambda s, h: (s, h // 2)),
            spec(lambda s, h: (s, h)),
            spec(lambda s, h: (s, h % 2)),
            spec(lambda s, h: (s, h)),
        ],
        out_specs=spec(lambda s, h: (s, h)),
        out_shape=jax.ShapeDtypeStruct((tokens, width), jnp.bfloat16),
        cost_estimate=pl.CostEstimate(flops=4 * tokens * seq_len * width, bytes_accessed=10 * tokens * width, transcendentals=0),
        name="attention_core",
    )(q_nope, q_rot, k_nope, k_rot, values)


def swap_halves(cols, half):
    rows, width = cols.shape
    pairs = cols.reshape(rows, width // (2 * half), 2, half)
    return pairs[:, :, ::-1, :].reshape(rows, width)


def attention(normed, w_dq, g_q, w_uq, w_dkv, g_kv, w_uk, w_uv, w_out, seq_len, rope_dim):
    tokens = normed.shape[0]
    num_seqs = tokens // seq_len
    kv_rank, heads_nope = w_uk.shape
    half = rope_dim // 2
    heads = (w_uq.shape[1] - heads_nope) // rope_dim
    nope_dim = heads_nope // heads
    positions = jnp.arange(seq_len)
    inv_freq = 1.0 / (ROPE_BASE ** (jnp.arange(0, rope_dim, 2).astype(jnp.float32) / rope_dim))
    angles = positions.astype(jnp.float32)[:, None] * inv_freq[None, :]
    cos_t, sin_t = jnp.cos(angles), jnp.sin(angles)
    cos_w = jnp.concatenate([cos_t, cos_t], axis=1)
    sin_w = jnp.concatenate([-sin_t, sin_t], axis=1)

    q_lat = rms_norm(mm(normed, w_dq).astype(jnp.bfloat16), g_q)
    q_nope = mm(q_lat, w_uq[:, :heads_nope]).astype(jnp.bfloat16)
    w_pe = w_uq[:, heads_nope:]
    q_pe = mm(q_lat, w_pe).astype(jnp.bfloat16)
    q_sw = mm(q_lat, swap_halves(w_pe, half)).astype(jnp.bfloat16)

    def turn(vals, swapped):
        reps = vals.shape[1] // rope_dim
        cos_r, sin_r = jnp.tile(cos_w, (num_seqs, reps)), jnp.tile(sin_w, (num_seqs, reps))
        return (vals.astype(jnp.float32) * cos_r + swapped.astype(jnp.float32) * sin_r).astype(jnp.bfloat16)

    q_rot = turn(q_pe, q_sw)
    kv_all = mm(normed, w_dkv).astype(jnp.bfloat16)
    latent = rms_norm(kv_all[:, :kv_rank], g_kv)
    k_pe = kv_all[:, kv_rank : kv_rank + rope_dim]
    k_rot = turn(k_pe, kv_all[:, kv_rank + rope_dim :])
    blank = jnp.zeros_like(k_rot)
    k_rot = jnp.concatenate([k_rot, blank, blank, k_rot], axis=1)
    k_nope = mm(latent, w_uk).astype(jnp.bfloat16)
    values = mm(latent, w_uv).astype(jnp.bfloat16)
    attended = attention_core(q_nope, q_rot, k_nope, k_rot, values, seq_len, (nope_dim + rope_dim) ** -0.5)
    return mm(attended, w_out).astype(jnp.bfloat16)


def moe_kernel(first, last, experts, meta_ref, tab_ref, rank_ref, gate_ref, u_hbm, *refs):
    if first:
        h_hbm, s_hbm, w_hbm, *refs = refs
    else:
        a_hbm, w_hbm, *refs = refs
    o_hbm, u_vm, acc, wbuf, xbuf, obuf, st_a, st_b, wsem, sem_a, sem_b, asem = refs
    tokens, width = u_hbm.shape
    pieces = width // LANES
    inter = w_hbm.shape[2]
    tile_lo, tile_hi, rank_lo = meta_ref[0], meta_ref[1], meta_ref[2]
    blocks = tokens // TILE

    def w_copy(expert):
        slot = lax.rem(expert, 2)
        return pltpu.make_async_copy(w_hbm.at[expert], wbuf.at[slot], wsem.at[slot])

    w_copy(0).start()
    if not first:
        acc_in = pltpu.make_async_copy(a_hbm, acc.at[pl.ds(0, tokens * pieces), :], asem)
        acc_in.start()

    def spread(dst, base, block):
        for j in range(pieces):
            dst[pl.ds(base * pieces + j, TILE, stride=pieces), :] = block[:, j * LANES : (j + 1) * LANES]

    def load_rows(src, stage, sem, step):
        return pltpu.make_async_copy(src.at[pl.ds(step * TILE, TILE), :], stage.at[lax.rem(step, 2)], sem.at[lax.rem(step, 2)])

    load_rows(u_hbm, st_a, sem_a, 0).start()

    @pl.loop(0, blocks)
    def _(step):
        @pl.when(step + 1 < blocks)
        def _():
            load_rows(u_hbm, st_a, sem_a, step + 1).start()

        load_rows(u_hbm, st_a, sem_a, step).wait()
        spread(u_vm, step * TILE, st_a[lax.rem(step, 2)].astype(jnp.float32))

    u_vm[pl.ds(tokens * pieces, 8), :] = jnp.zeros((8, LANES), jnp.float32)
    if first:
        load_rows(h_hbm, st_a, sem_a, 0).start()
        load_rows(s_hbm, st_b, sem_b, 0).start()

        @pl.loop(0, blocks)
        def _(step):
            @pl.when(step + 1 < blocks)
            def _():
                load_rows(h_hbm, st_a, sem_a, step + 1).start()
                load_rows(s_hbm, st_b, sem_b, step + 1).start()

            load_rows(h_hbm, st_a, sem_a, step).wait()
            load_rows(s_hbm, st_b, sem_b, step).wait()
            slot = lax.rem(step, 2)
            spread(acc, step * TILE, st_a[slot].astype(jnp.float32) + st_b[slot].astype(jnp.float32))
    else:
        acc_in.wait()
    acc[pl.ds(tokens * pieces, 8), :] = jnp.zeros((8, LANES), jnp.float32)

    def row_of(slot):
        return pl.ds(pl.multiple_of((slot >> 3) << 3, 8), 8)

    def tile_step(tile, current):
        expert = rank_ref[tile] - rank_lo

        @pl.loop(current + 1, expert + 1)
        def _(e):
            w_copy(e).wait()

            @pl.when(e + 1 < experts)
            def _():
                w_copy(e + 1).start()

        base = tile * TILE

        @pl.loop(0, TILE // 16)
        def _(group):
            for r in range(16):
                slot = tab_ref[base + group * 16 + r]
                xbuf[pl.ds(group * 16 + r, pieces, stride=PITCH), :] = u_vm[row_of(slot), :]

        rows = jnp.concatenate([xbuf[j * PITCH : j * PITCH + TILE, :].astype(jnp.bfloat16) for j in range(pieces)], axis=1)
        weights = wbuf.at[lax.rem(expert, 2)]
        gate = mm(rows, weights[0:width, :])
        upper = mm(rows, weights[width : 2 * width, :])
        hidden = (jax.nn.silu(gate) * upper).astype(jnp.bfloat16)
        for b in range(width // inter):
            out = mm(hidden, weights[2 * width + b * inter : 2 * width + (b + 1) * inter, :])
            out = out.astype(jnp.bfloat16).astype(jnp.float32)
            for j in range(inter // LANES):
                piece = b * (inter // LANES) + j
                obuf[piece * PITCH : piece * PITCH + TILE, :] = out[:, j * LANES : (j + 1) * LANES]

        @pl.loop(0, TILE // 8)
        def _(group):
            slots = [tab_ref[base + group * 8 + r] for r in range(8)]
            gates = [gate_ref[jnp.minimum(s, tokens * pieces - 1)] for s in slots]
            sums = [
                acc[row_of(s), :] + g * obuf[pl.ds(group * 8 + r, pieces, stride=PITCH), :]
                for r, (s, g) in enumerate(zip(slots, gates))
            ]
            for s, total in zip(slots, sums):
                acc[row_of(s), :] = total

        return expert

    final = lax.fori_loop(tile_lo, tile_hi, tile_step, jnp.int32(-1))

    @pl.loop(final + 1, experts)
    def _(e):
        w_copy(e).wait()

        @pl.when(e + 1 < experts)
        def _():
            w_copy(e + 1).start()

    if last:

        def store_rows(step):
            return pltpu.make_async_copy(st_a.at[lax.rem(step, 2)], o_hbm.at[pl.ds(step * TILE, TILE), :], sem_a.at[lax.rem(step, 2)])

        @pl.loop(0, blocks)
        def _(step):
            @pl.when(step >= 2)
            def _():
                store_rows(step - 2).wait()

            parts = [acc[pl.ds(step * TILE * pieces + j, TILE, stride=pieces), :].astype(jnp.bfloat16) for j in range(pieces)]
            st_a[lax.rem(step, 2)] = jnp.concatenate(parts, axis=1)
            store_rows(step).start()

        store_rows(blocks - 2).wait()
        store_rows(blocks - 1).wait()
    else:
        acc_out = pltpu.make_async_copy(acc.at[pl.ds(0, tokens * pieces), :], o_hbm, asem)
        acc_out.start()
        acc_out.wait()


def moe_call(first, last, meta, table, ranks, gates, u_norm, extra, weights):
    tokens, width = u_norm.shape
    pieces = width // LANES
    experts, wrows, inter = weights.shape
    smem = pl.BlockSpec(memory_space=pltpu.SMEM)
    hbm = pl.BlockSpec(memory_space=pl.ANY)
    scratch = [
        pltpu.VMEM((tokens * pieces + 8, LANES), jnp.float32),
        pltpu.VMEM((tokens * pieces + 8, LANES), jnp.float32),
        pltpu.VMEM((2, wrows, inter), jnp.bfloat16),
        pltpu.VMEM((pieces * PITCH, LANES), jnp.float32),
        pltpu.VMEM((pieces * PITCH, LANES), jnp.float32),
        pltpu.VMEM((2, TILE, width), jnp.bfloat16),
        pltpu.VMEM((2, TILE, width), jnp.bfloat16),
        pltpu.SemaphoreType.DMA((2,)),
        pltpu.SemaphoreType.DMA((2,)),
        pltpu.SemaphoreType.DMA((2,)),
        pltpu.SemaphoreType.DMA,
    ]
    out_shape = jax.ShapeDtypeStruct((tokens, width), jnp.bfloat16) if last else jax.ShapeDtypeStruct((tokens * pieces, LANES), jnp.float32)
    rows = experts * tokens // 8
    return pl.pallas_call(
        functools.partial(moe_kernel, first, last, experts),
        in_specs=[smem] * 4 + [hbm] * (2 + len(extra)),
        out_specs=hbm,
        out_shape=out_shape,
        scratch_shapes=scratch,
        compiler_params=pltpu.CompilerParams(vmem_limit_bytes=VMEM_LIMIT),
        cost_estimate=pl.CostEstimate(flops=2 * rows * wrows * inter, bytes_accessed=2 * experts * wrows * inter, transcendentals=0),
        name="routed_experts",
    )(meta, table, ranks, gates, u_norm, *extra, weights)


def route_plan(choice_ids, num_experts, groups):
    tokens, num_top = choice_ids.shape
    local = num_experts // groups
    device, index = choice_ids // local, choice_ids % local
    rank = jnp.zeros_like(choice_ids)
    low = 0
    for size in CHUNKS:
        rank = jnp.where((index >= low) & (index < low + size), low * groups + device * size + index - low, rank)
        low += size
    hits = rank[:, :, None] == jnp.arange(num_experts)[None, None, :]
    counts = jnp.sum(hits.astype(jnp.int32), axis=(0, 1))
    slots = jnp.arange(tokens)[:, None] * num_top + jnp.arange(num_top)[None, :]
    keys = (rank * 65536 + slots).reshape(-1)
    spare = jnp.arange(TILE)[None, :] < ((-counts) % TILE)[:, None]
    dummy = tokens * num_top
    fill = jnp.where(spare, jnp.arange(num_experts)[:, None] * 65536 + dummy, num_experts * 65536 + dummy)
    ordered = jnp.sort(jnp.concatenate([keys, fill.reshape(-1)]), stable=False)
    tiles = (counts + TILE - 1) // TILE
    ends = jnp.cumsum(tiles)
    metas = []
    low = 0
    for size in CHUNKS:
        begin = ends[low * groups - 1] if low else jnp.int32(0)
        low += size
        metas.append(jnp.stack([begin, ends[low * groups - 1], jnp.int32((low - size) * groups), jnp.int32(0)]).astype(jnp.int32))
    return ordered & 65535, ordered[::TILE] // 65536, metas


def solution(mesh):
    groups = mesh.shape[AXIS]
    rows_spec = P(AXIS, None)
    vec_spec = P(AXIS)
    full_spec = P(None, None)
    cube_spec = P(AXIS, None, None)
    in_specs = (cube_spec, vec_spec, rows_spec, rows_spec, rows_spec, vec_spec, rows_spec, vec_spec, rows_spec, rows_spec, vec_spec, rows_spec, rows_spec, rows_spec, vec_spec, full_spec, cube_spec, cube_spec, cube_spec, full_spec, full_spec, full_spec, cube_spec)

    def gather(shard):
        return lax.all_gather(shard, AXIS, axis=0, tiled=True)

    def local(x_resid, g_mlp, w_gate, w_up, w_down, g_attn, w_dq, g_q, w_uq, w_dkv, g_kv, w_uk, w_uv, w_out, g_moe, w_router, we_gate, we_up, we_down, ws_gate, ws_up, ws_down, expert_ids):
        num_seqs, seq_len, width = x_resid.shape
        tokens = num_seqs * seq_len
        num_experts = w_router.shape[0]
        inter = we_gate.shape[2]
        flat_x = x_resid.reshape(tokens, width)
        choice_ids = expert_ids.reshape(tokens, expert_ids.shape[2])

        gains = [g_mlp, g_attn, g_q, g_kv, g_moe]
        sizes = [g.shape[0] for g in gains]
        packed = lax.all_gather(jnp.concatenate(gains), AXIS, axis=0, tiled=False)
        offs = [sum(sizes[:i]) for i in range(len(sizes))]
        g_mlp, g_attn, g_q, g_kv, g_moe = [packed[:, o : o + s].reshape(-1) for o, s in zip(offs, sizes)]

        inner = w_gate.shape[1]
        gate_up = gather(jnp.concatenate([w_gate, w_up], axis=1))
        down = gather(w_down)
        kv_rank = w_uk.shape[0] * groups
        rope_dim = w_dkv.shape[1] - kv_rank
        heads = (w_uq.shape[1] - w_uk.shape[1]) // rope_dim
        nope_dim = w_uk.shape[1] // heads
        per_head = w_uq.reshape(w_uq.shape[0], heads, nope_dim + rope_dim)
        uq_local = jnp.concatenate([per_head[:, :, :nope_dim].reshape(-1, heads * nope_dim), per_head[:, :, nope_dim:].reshape(-1, heads * rope_dim)], axis=1)
        dkv_local = jnp.concatenate([w_dkv, swap_halves(w_dkv[:, kv_rank:], rope_dim // 2)], axis=1)
        shards = [w_dq, dkv_local, uq_local, w_uk, w_uv, w_out]
        blocks = [to_blocks(s) for s in shards]
        attn_w = gather(jnp.concatenate(blocks, axis=0)[None])
        starts = [sum(b.shape[0] for b in blocks[:i]) for i in range(len(blocks))]
        w_dq, w_dkv, w_uq, w_uk, w_uv, w_out = [from_blocks(attn_w, st, s.shape[0], s.shape[1]) for st, s in zip(starts, shards)]

        down_blocks = we_down.reshape(we_down.shape[0], inter, width // inter, inter).transpose(0, 2, 1, 3).reshape(we_down.shape[0], width, inter)
        pack = jnp.concatenate([we_gate, we_up, down_blocks], axis=1)
        expert_w = []
        low = 0
        for size in CHUNKS:
            expert_w.append(gather(pack[low : low + size]))
            low += size

        table, ranks, metas = route_plan(choice_ids, num_experts, groups)

        normed = rms_norm(flat_x, g_mlp)
        hidden = (jax.nn.silu(mm(normed, gate_up[:, :inner])) * mm(normed, gate_up[:, inner:])).astype(jnp.bfloat16)
        mlp_out = mm(hidden, down).astype(jnp.bfloat16)
        h_one = (flat_x.astype(jnp.float32) + mlp_out.astype(jnp.float32)).astype(jnp.bfloat16)
        attn_out = attention(rms_norm(h_one, g_attn), w_dq, g_q, w_uq, w_dkv, g_kv, w_uk, w_uv, w_out, seq_len, rope_dim)
        h_two = (h_one.astype(jnp.float32) + attn_out.astype(jnp.float32)).astype(jnp.bfloat16)
        u_norm = rms_norm(h_two, g_moe)
        logits = jnp.einsum("td,ed->te", u_norm.astype(jnp.float32), w_router, precision=lax.Precision.HIGHEST)
        scores = jax.nn.sigmoid(logits)
        hits = choice_ids[:, :, None] == jnp.arange(num_experts)[None, None, :]
        picked = jnp.sum(jnp.where(hits, scores[:, None, :], 0.0), axis=2)
        gates = (ROUTE_SCALE * picked / jnp.sum(picked, axis=1, keepdims=True)).reshape(-1)
        shared = swiglu(u_norm, ws_gate, ws_up, ws_down)

        total = None
        for i, weights in enumerate(expert_w):
            extra = (h_two, shared) if i == 0 else (total,)
            total = moe_call(i == 0, i == len(expert_w) - 1, metas[i], table, ranks, gates, u_norm, extra, weights)
        return total.reshape(num_seqs, seq_len, width)

    return jax.shard_map(local, mesh=mesh, in_specs=in_specs, out_specs=cube_spec, check_vma=False)
```

```python
import functools

import jax
import jax.numpy as jnp
from jax import lax
from jax.experimental import pallas as pl
from jax.experimental.pallas import tpu as pltpu
from jax.sharding import PartitionSpec as P


AXIS = "fsdp"
ROPE_BASE = 10000.0
EPS = 1e-6
ROUTE_SCALE = 2.5
TILE = 256
PITCH = TILE + 4
GROUP = 4
ORDER = (("D", 0), ("S", 5), ("D", 1), ("S", 5), ("D", 2), ("S", 5), ("D", 3), ("S", 5), ("G", 0), ("S", 6), ("U", 0), ("S", 5), ("G", 1), ("S", 5), ("U", 1), ("S", 5), ("G", 2), ("S", 6), ("U", 2), ("S", 5), ("G", 3), ("S", 6), ("U", 3), ("S", 6), ("H", 0))
LANES = 128
CHUNKS = (2, 2, 2, 2)
VMEM_LIMIT = 60 * 1024 * 1024


def rms_norm(vals, gain):
    vals = vals.astype(jnp.float32)
    scaled = vals * lax.rsqrt(jnp.mean(vals * vals, axis=-1, keepdims=True) + EPS)
    return (scaled * gain).astype(jnp.bfloat16)


def mm(lhs, rhs):
    return jnp.dot(lhs, rhs, preferred_element_type=jnp.float32)


def swiglu(rows, w_gate, w_up, w_down):
    hidden = (jax.nn.silu(mm(rows, w_gate)) * mm(rows, w_up)).astype(jnp.bfloat16)
    return mm(hidden, w_down).astype(jnp.bfloat16)


def to_blocks(shard):
    rows, cols = shard.shape
    return shard.reshape(rows, cols // LANES, LANES).transpose(1, 0, 2).reshape(-1, LANES)


def from_blocks(gathered, start, rows, cols):
    groups = gathered.shape[0]
    blocks = cols // LANES
    part = gathered[:, start : start + rows * blocks].reshape(groups, blocks, rows, LANES)
    return part.transpose(0, 2, 1, 3).reshape(groups * rows, cols)


def attn_kernel(scale, block, qn_ref, qp_ref, qs_ref, kn_ref, kr_ref, v_ref, cos_ref, sin_ref, o_ref):
    seq = qn_ref.shape[0]
    keys = jnp.concatenate([kn_ref[...], kr_ref[...]], axis=1)
    vals = v_ref[...]
    for start in range(0, seq, block):
        stop = start + block
        turned = qp_ref[start:stop, :].astype(jnp.float32) * cos_ref[start:stop, :] + qs_ref[start:stop, :].astype(jnp.float32) * sin_ref[start:stop, :]
        query = jnp.concatenate([qn_ref[start:stop, :], turned.astype(jnp.bfloat16)], axis=1)
        scores = lax.dot_general(query, keys[:stop], (((1,), (1,)), ((), ())), preferred_element_type=jnp.float32)
        row = lax.broadcasted_iota(jnp.int32, scores.shape, 0) + start
        col = lax.broadcasted_iota(jnp.int32, scores.shape, 1)
        scores = jnp.where(row >= col, scores * scale, -jnp.inf)
        expo = jnp.exp(scores - jnp.max(scores, axis=1, keepdims=True))
        probs = (expo * (1.0 / jnp.sum(expo, axis=1, keepdims=True))).astype(jnp.bfloat16)
        o_ref[start:stop, :] = mm(probs, vals[:stop]).astype(jnp.bfloat16)


def attention_core(q_nope, q_pe, k_nope, k_rot, values, cos_w, sin_w, seq_len, scale):
    tokens, width = q_nope.shape
    seqs, heads = tokens // seq_len, width // LANES
    spec = lambda fn: pl.BlockSpec((seq_len, LANES), fn)
    return pl.pallas_call(
        functools.partial(attn_kernel, scale, 256),
        grid=(seqs, heads),
        in_specs=[
            spec(lambda s, h: (s, h)),
            spec(lambda s, h: (s, h // 2)),
            spec(lambda s, h: (s, heads // 2 + h // 2)),
            spec(lambda s, h: (s, h)),
            spec(lambda s, h: (s, h % 2)),
            spec(lambda s, h: (s, h)),
            spec(lambda s, h: (0, 0)),
            spec(lambda s, h: (0, 0)),
        ],
        out_specs=spec(lambda s, h: (s, h)),
        out_shape=jax.ShapeDtypeStruct((tokens, width), jnp.bfloat16),
        cost_estimate=pl.CostEstimate(flops=4 * tokens * seq_len * width, bytes_accessed=10 * tokens * width, transcendentals=0),
        name="attention_core",
    )(q_nope, q_pe, q_pe, k_nope, k_rot, values, cos_w, sin_w)


def swap_halves(cols, half):
    rows, width = cols.shape
    pairs = cols.reshape(rows, width // (2 * half), 2, half)
    return pairs[:, :, ::-1, :].reshape(rows, width)


def attention(normed, w_dq, g_q, w_uq, w_dkv, g_kv, w_uk, w_uv, w_out, seq_len, rope_dim):
    tokens = normed.shape[0]
    num_seqs = tokens // seq_len
    kv_rank, heads_nope = w_uk.shape
    half = rope_dim // 2
    heads = (w_uq.shape[1] - heads_nope) // rope_dim
    nope_dim = heads_nope // heads
    positions = jnp.arange(seq_len)
    inv_freq = 1.0 / (ROPE_BASE ** (jnp.arange(0, rope_dim, 2).astype(jnp.float32) / rope_dim))
    angles = positions.astype(jnp.float32)[:, None] * inv_freq[None, :]
    cos_t, sin_t = jnp.cos(angles), jnp.sin(angles)
    cos_w = jnp.concatenate([cos_t] * 4, axis=1)
    sin_w = jnp.concatenate([-sin_t, sin_t] * 2, axis=1)
    q_lat = rms_norm(mm(normed, w_dq).astype(jnp.bfloat16), g_q)
    q_nope = mm(q_lat, w_uq[:, :heads_nope]).astype(jnp.bfloat16)
    w_pe = w_uq[:, heads_nope:]
    q_pe = mm(q_lat, jnp.concatenate([w_pe, swap_halves(w_pe, half)], axis=1)).astype(jnp.bfloat16)

    kv_all = mm(normed, w_dkv).astype(jnp.bfloat16)
    latent = rms_norm(kv_all[:, :kv_rank], g_kv)
    k_pe = kv_all[:, kv_rank:].reshape(num_seqs, seq_len, 2 * rope_dim).astype(jnp.float32)
    k_rot = k_pe[..., :rope_dim] * cos_w[None, :, :rope_dim] + k_pe[..., rope_dim:] * sin_w[None, :, :rope_dim]
    k_rot = k_rot.astype(jnp.bfloat16).reshape(tokens, rope_dim)
    blank = jnp.zeros_like(k_rot)
    k_rot = jnp.concatenate([k_rot, blank, blank, k_rot], axis=1)
    k_nope = mm(latent, w_uk).astype(jnp.bfloat16)
    values = mm(latent, w_uv).astype(jnp.bfloat16)
    attended = attention_core(q_nope, q_pe, k_nope, k_rot, values, cos_w, sin_w, seq_len, (nope_dim + rope_dim) ** -0.5)
    return mm(attended, w_out).astype(jnp.bfloat16)


def moe_kernel(first, last, meta_ref, rank_ref, gate_ref, tab_hbm, u_hbm, *refs):
    if first:
        h_hbm, s_hbm, w_hbm, *refs = refs
    else:
        a_hbm, w_hbm, *refs = refs
    o_hbm, u_vm, acc, wbuf, *refs = refs
    x_bufs, o_bufs, h_bufs, t_next, t_prev, s_prev = (refs[i : i + 2] for i in range(0, 12, 2))
    st_a, st_b, wsem, sem_a, sem_b, asem, lsem = refs[12:]
    tokens, width = u_hbm.shape
    pieces = width // LANES
    inter = w_hbm.shape[2]
    tile_lo, tile_hi, experts = meta_ref[0], meta_ref[1], meta_ref[2]
    blocks = tokens // TILE

    def w_copy(order):
        slot = lax.rem(order, 3)
        return pltpu.make_async_copy(w_hbm.at[meta_ref[3 + order]], wbuf.at[slot], wsem.at[slot])

    @pl.when(experts > 0)
    def _():
        w_copy(0).start()

    if not first:
        acc_in = pltpu.make_async_copy(a_hbm, acc.at[pl.ds(0, tokens * pieces), :], asem)
        acc_in.start()

    def spread(dst, base, block):
        for j in range(pieces):
            dst[pl.ds(base * pieces + j, TILE, stride=pieces), :] = block[:, j * LANES : (j + 1) * LANES]

    def load_rows(src, stage, sem, step):
        return pltpu.make_async_copy(src.at[pl.ds(step * TILE, TILE), :], stage.at[lax.rem(step, 2)], sem.at[lax.rem(step, 2)])

    load_rows(u_hbm, st_a, sem_a, 0).start()

    @pl.loop(0, blocks)
    def _(step):
        @pl.when(step + 1 < blocks)
        def _():
            load_rows(u_hbm, st_a, sem_a, step + 1).start()

        load_rows(u_hbm, st_a, sem_a, step).wait()
        spread(u_vm, step * TILE, st_a[lax.rem(step, 2)].astype(jnp.float32))

    u_vm[pl.ds(tokens * pieces, 8), :] = jnp.zeros((8, LANES), jnp.float32)
    if first:
        load_rows(h_hbm, st_a, sem_a, 0).start()
        load_rows(s_hbm, st_b, sem_b, 0).start()

        @pl.loop(0, blocks)
        def _(step):
            @pl.when(step + 1 < blocks)
            def _():
                load_rows(h_hbm, st_a, sem_a, step + 1).start()
                load_rows(s_hbm, st_b, sem_b, step + 1).start()

            load_rows(h_hbm, st_a, sem_a, step).wait()
            load_rows(s_hbm, st_b, sem_b, step).wait()
            slot = lax.rem(step, 2)
            spread(acc, step * TILE, st_a[slot].astype(jnp.float32) + st_b[slot].astype(jnp.float32))
    else:
        acc_in.wait()
    acc[pl.ds(tokens * pieces, 8), :] = jnp.zeros((8, LANES), jnp.float32)

    idle = tab_hbm.shape[0] - 1
    count = tile_hi - tile_lo

    def tile_at(step):
        return jnp.where((step >= 0) & (step < count), tile_lo + step, idle)

    def list_copies(step, parity):
        ahead, behind = tab_hbm.at[tile_at(step + 1)], tab_hbm.at[tile_at(step - 2)]
        return (
            pltpu.make_async_copy(ahead.at[0], t_next[parity], lsem.at[parity, 0]),
            pltpu.make_async_copy(behind.at[0], t_prev[parity], lsem.at[parity, 1]),
            pltpu.make_async_copy(behind.at[1], s_prev[parity], lsem.at[parity, 2]),
        )

    def row_at(offset):
        return pl.ds(pl.multiple_of(offset, pieces), pieces)

    def order_at(step):
        return jnp.where((step >= 0) & (step < count), rank_ref[tile_at(step)], 0)

    depth = 2 * LANES
    half = TILE // 2

    def column(buf, j):
        parts = [buf[pl.ds(j * PITCH + odd, half, stride=2), :] for odd in (0, 1)]
        return jnp.concatenate(parts, axis=0)

    def half_step(step, parity):
        x_now, x_next = x_bufs[parity], x_bufs[1 - parity]
        h_now, h_prev = h_bufs[parity], h_bufs[1 - parity]
        o_now, o_prev = o_bufs[parity], o_bufs[1 - parity]
        ahead, behind, slots = t_next[parity], t_prev[parity], s_prev[parity]
        for copy in list_copies(step + 1, 1 - parity):
            copy.start()
        mine, before = order_at(step), order_at(step - 1)

        @pl.when((step < count) & ((step == 0) | (mine != before)))
        def _():
            w_copy(mine).wait()

            @pl.when(mine + 1 < experts)
            def _():
                w_copy(mine + 1).start()

        for copy in list_copies(step, parity):
            copy.wait()

        def side_work(low, high):
            for start in range(low, high, GROUP):
                for r in range(start, start + GROUP):
                    x_next[pl.ds(r, pieces, stride=PITCH), :] = u_vm[row_at(ahead[r]), :]
                spots = [behind[r] for r in range(start, start + GROUP)]
                sums = [acc[row_at(t), :] + gate_ref[slots[start + r]] * o_prev[pl.ds(start + r, pieces, stride=PITCH), :] for r, t in enumerate(spots)]
                for r, total in enumerate(sums):
                    acc[row_at(behind[start + r]), :] = total

        w_now, w_prev = wbuf.at[lax.rem(mine, 3)], wbuf.at[lax.rem(before, 3)]
        sums, parts = {}, {}
        done = 0
        for kind, k in ORDER:
            if kind in "GU":
                if k not in parts:
                    parts[k] = jnp.concatenate([column(x_now, 2 * k).astype(jnp.bfloat16), column(x_now, 2 * k + 1).astype(jnp.bfloat16)], axis=1)
                low = (0 if kind == "G" else width) + k * depth
                term = mm(parts[k], w_now[low : low + depth, :])
                sums[kind] = term if k == 0 else sums[kind] + term
            elif kind == "D":
                low = 2 * width + k * inter
                out = mm(h_prev[...], w_prev[low : low + inter, :]).astype(jnp.bfloat16).astype(jnp.float32)
                for j in range(inter // LANES):
                    for odd in (0, 1):
                        at = pl.ds((k * (inter // LANES) + j) * PITCH + odd, half, stride=2)
                        o_now[at, :] = out[odd * half : (odd + 1) * half, j * LANES : (j + 1) * LANES]
            elif kind == "S":
                side_work(done, done + k * GROUP)
                done += k * GROUP
            else:
                h_now[...] = (jax.nn.silu(sums["G"]) * sums["U"]).astype(jnp.bfloat16)
        side_work(done, TILE)

    first_list = pltpu.make_async_copy(tab_hbm.at[tile_at(0), 0], t_next[1], lsem.at[1, 0])
    first_list.start()
    for copy in list_copies(0, 0):
        copy.start()
    first_list.wait()
    for r in range(TILE):
        x_bufs[0][pl.ds(r, pieces, stride=PITCH), :] = u_vm[row_at(t_next[1][r]), :]

    pairs = (count + 3) // 2

    @pl.loop(0, pairs)
    def _(i):
        half_step(2 * i, 0)
        half_step(2 * i + 1, 1)

    for copy in list_copies(2 * pairs, 0):
        copy.wait()

    if last:

        def store_rows(step):
            return pltpu.make_async_copy(st_a.at[lax.rem(step, 2)], o_hbm.at[pl.ds(step * TILE, TILE), :], sem_a.at[lax.rem(step, 2)])

        @pl.loop(0, blocks)
        def _(step):
            @pl.when(step >= 2)
            def _():
                store_rows(step - 2).wait()

            parts = [acc[pl.ds(step * TILE * pieces + j, TILE, stride=pieces), :].astype(jnp.bfloat16) for j in range(pieces)]
            st_a[lax.rem(step, 2)] = jnp.concatenate(parts, axis=1)
            store_rows(step).start()

        store_rows(blocks - 2).wait()
        store_rows(blocks - 1).wait()
    else:
        acc_out = pltpu.make_async_copy(acc.at[pl.ds(0, tokens * pieces), :], o_hbm, asem)
        acc_out.start()
        acc_out.wait()


def moe_call(first, last, meta, table, ranks, gates, u_norm, extra, weights):
    tokens, width = u_norm.shape
    pieces = width // LANES
    experts, wrows, inter = weights.shape
    smem = pl.BlockSpec(memory_space=pltpu.SMEM)
    hbm = pl.BlockSpec(memory_space=pl.ANY)
    scratch = [
        pltpu.VMEM((tokens * pieces + 8, LANES), jnp.float32),
        pltpu.VMEM((tokens * pieces + 8, LANES), jnp.float32),
        pltpu.VMEM((3, wrows, inter), jnp.bfloat16),
        *[pltpu.VMEM((pieces * PITCH, LANES), jnp.float32)] * 4,
        *[pltpu.VMEM((TILE, inter), jnp.bfloat16)] * 2,
        *[pltpu.SMEM((TILE,), jnp.int32)] * 6,
        pltpu.VMEM((2, TILE, width), jnp.bfloat16),
        pltpu.VMEM((2, TILE, width), jnp.bfloat16),
        pltpu.SemaphoreType.DMA((3,)),
        pltpu.SemaphoreType.DMA((2,)),
        pltpu.SemaphoreType.DMA((2,)),
        pltpu.SemaphoreType.DMA,
        pltpu.SemaphoreType.DMA((2, 3)),
    ]
    out_shape = jax.ShapeDtypeStruct((tokens, width), jnp.bfloat16) if last else jax.ShapeDtypeStruct((tokens * pieces, LANES), jnp.float32)
    rows = experts * tokens // 8
    return pl.pallas_call(
        functools.partial(moe_kernel, first, last),
        in_specs=[smem] * 3 + [hbm] * (3 + len(extra)),
        out_specs=hbm,
        out_shape=out_shape,
        scratch_shapes=scratch,
        compiler_params=pltpu.CompilerParams(vmem_limit_bytes=VMEM_LIMIT),
        cost_estimate=pl.CostEstimate(flops=2 * rows * wrows * inter, bytes_accessed=2 * experts * wrows * inter, transcendentals=0),
        name="routed_experts",
    )(meta, ranks, gates, table, u_norm, *extra, weights)


def route_plan(choice_ids, num_experts, groups):
    tokens, num_top = choice_ids.shape
    local = num_experts // groups
    device, index = choice_ids // local, choice_ids % local
    rank = jnp.zeros_like(choice_ids)
    low = 0
    for size in CHUNKS:
        rank = jnp.where((index >= low) & (index < low + size), low * groups + device * size + index - low, rank)
        low += size
    hits = rank[:, :, None] == jnp.arange(num_experts)[None, None, :]
    counts = jnp.sum(hits.astype(jnp.int32), axis=(0, 1))
    slots = jnp.arange(tokens)[:, None] * num_top + jnp.arange(num_top)[None, :]
    keys = (rank * 65536 + slots).reshape(-1)
    spare = jnp.arange(TILE)[None, :] < ((-counts) % TILE)[:, None]
    dummy = tokens * num_top
    fill = jnp.where(spare, jnp.arange(num_experts)[:, None] * 65536 + dummy, num_experts * 65536 + dummy)
    ordered = jnp.sort(jnp.concatenate([keys, fill.reshape(-1)]), stable=False)
    tiles = (counts + TILE - 1) // TILE
    spans = [(sum(CHUNKS[:i]) * groups, sum(CHUNKS[: i + 1]) * groups) for i in range(len(CHUNKS))]
    experts = jnp.arange(num_experts)
    chunk = sum((experts >= low).astype(jnp.int32) for low, _ in spans) - 1
    used = counts > 0
    ahead = (chunk[:, None] == chunk[None, :]) & (experts[None, :] < experts[:, None])
    order = jnp.sum(jnp.where(ahead & used[None, :], 1, 0), axis=1)
    start = jnp.array([low for low, _ in spans])
    stop = jnp.array([high for _, high in spans])
    member = (experts[None, :] >= start[:, None]) & (experts[None, :] < stop[:, None]) & used[None, :]
    names = jnp.sum(jnp.where(member[:, None, :] & (order[None, None, :] == experts[None, :, None]), experts[None, None, :] - start[:, None, None], 0), axis=2)
    first = jnp.sum(jnp.where(experts[None, :] < start[:, None], tiles[None, :], 0), axis=1)
    final = jnp.sum(jnp.where(experts[None, :] < stop[:, None], tiles[None, :], 0), axis=1)
    metas = jnp.concatenate([jnp.stack([first, final, jnp.sum(member.astype(jnp.int32), axis=1)], axis=1), names], axis=1).astype(jnp.int32)
    ranks = ordered[::TILE] // 65536
    orders = jnp.sum(jnp.where(ranks[:, None] == experts[None, :], order[None, :], 0), axis=1)
    low = ordered & 65535
    table = jnp.stack([(low & ~7).reshape(-1, TILE), low.reshape(-1, TILE)], axis=1)
    return table, orders, metas


def solution(mesh):
    groups = mesh.shape[AXIS]
    rows_spec = P(AXIS, None)
    vec_spec = P(AXIS)
    full_spec = P(None, None)
    cube_spec = P(AXIS, None, None)
    in_specs = (cube_spec, vec_spec, rows_spec, rows_spec, rows_spec, vec_spec, rows_spec, vec_spec, rows_spec, rows_spec, vec_spec, rows_spec, rows_spec, rows_spec, vec_spec, full_spec, cube_spec, cube_spec, cube_spec, full_spec, full_spec, full_spec, cube_spec)

    def gather(shard):
        return lax.all_gather(shard, AXIS, axis=0, tiled=True)

    def local(x_resid, g_mlp, w_gate, w_up, w_down, g_attn, w_dq, g_q, w_uq, w_dkv, g_kv, w_uk, w_uv, w_out, g_moe, w_router, we_gate, we_up, we_down, ws_gate, ws_up, ws_down, expert_ids):
        num_seqs, seq_len, width = x_resid.shape
        tokens = num_seqs * seq_len
        num_experts = w_router.shape[0]
        inter = we_gate.shape[2]
        flat_x = x_resid.reshape(tokens, width)
        choice_ids = expert_ids.reshape(tokens, expert_ids.shape[2])

        gains = [g_mlp, g_attn, g_q, g_kv, g_moe]
        sizes = [g.shape[0] for g in gains]
        packed = lax.all_gather(jnp.concatenate(gains), AXIS, axis=0, tiled=False)
        offs = [sum(sizes[:i]) for i in range(len(sizes))]
        g_mlp, g_attn, g_q, g_kv, g_moe = [packed[:, o : o + s].reshape(-1) for o, s in zip(offs, sizes)]

        inner = w_gate.shape[1]
        gate_up = gather(jnp.concatenate([w_gate, w_up], axis=1))
        down = gather(w_down)
        kv_rank = w_uk.shape[0] * groups
        rope_dim = w_dkv.shape[1] - kv_rank
        heads = (w_uq.shape[1] - w_uk.shape[1]) // rope_dim
        nope_dim = w_uk.shape[1] // heads
        per_head = w_uq.reshape(w_uq.shape[0], heads, nope_dim + rope_dim)
        uq_local = jnp.concatenate([per_head[:, :, :nope_dim].reshape(-1, heads * nope_dim), per_head[:, :, nope_dim:].reshape(-1, heads * rope_dim)], axis=1)
        dkv_local = jnp.concatenate([w_dkv, swap_halves(w_dkv[:, kv_rank:], rope_dim // 2)], axis=1)
        shards = [w_dq, dkv_local, uq_local, w_uk, w_uv, w_out]
        blocks = [to_blocks(s) for s in shards]
        attn_w = gather(jnp.concatenate(blocks, axis=0)[None])
        starts = [sum(b.shape[0] for b in blocks[:i]) for i in range(len(blocks))]
        w_dq, w_dkv, w_uq, w_uk, w_uv, w_out = [from_blocks(attn_w, st, s.shape[0], s.shape[1]) for st, s in zip(starts, shards)]

        down_blocks = we_down.reshape(we_down.shape[0], inter, width // inter, inter).transpose(0, 2, 1, 3).reshape(we_down.shape[0], width, inter)
        pack = jnp.concatenate([we_gate, we_up, down_blocks], axis=1)
        expert_w = []
        low = 0
        for size in CHUNKS:
            expert_w.append(gather(pack[low : low + size]))
            low += size

        table, ranks, metas = route_plan(choice_ids, num_experts, groups)

        normed = rms_norm(flat_x, g_mlp)
        hidden = (jax.nn.silu(mm(normed, gate_up[:, :inner])) * mm(normed, gate_up[:, inner:])).astype(jnp.bfloat16)
        mlp_out = mm(hidden, down).astype(jnp.bfloat16)
        h_one = (flat_x.astype(jnp.float32) + mlp_out.astype(jnp.float32)).astype(jnp.bfloat16)
        attn_out = attention(rms_norm(h_one, g_attn), w_dq, g_q, w_uq, w_dkv, g_kv, w_uk, w_uv, w_out, seq_len, rope_dim)
        h_two = (h_one.astype(jnp.float32) + attn_out.astype(jnp.float32)).astype(jnp.bfloat16)
        u_norm = rms_norm(h_two, g_moe)
        logits = jnp.einsum("td,ed->te", u_norm.astype(jnp.float32), w_router, precision=lax.Precision.HIGHEST)
        scores = jax.nn.sigmoid(logits)
        hits = choice_ids[:, :, None] == jnp.arange(num_experts)[None, None, :]
        picked = jnp.sum(jnp.where(hits, scores[:, None, :], 0.0), axis=2)
        gates = (ROUTE_SCALE * picked / jnp.sum(picked, axis=1, keepdims=True)).reshape(-1)
        gates = jnp.concatenate([gates, jnp.zeros((8,), jnp.float32)])
        shared = swiglu(u_norm, ws_gate, ws_up, ws_down)

        total = None
        for i, weights in enumerate(expert_w):
            extra = (h_two, shared) if i == 0 else (total,)
            total = moe_call(i == 0, i == len(expert_w) - 1, metas[i], table, ranks, gates, u_norm, extra, weights)
        return total.reshape(num_seqs, seq_len, width)

    return jax.shard_map(local, mesh=mesh, in_specs=in_specs, out_specs=cube_spec, check_vma=False)
```

```python
import functools

import jax
import jax.numpy as jnp
from jax import lax
from jax.experimental import pallas as pl
from jax.experimental.pallas import tpu as pltpu
from jax.sharding import PartitionSpec as P


AXIS = "fsdp"
ROPE_BASE = 10000.0
EPS = 1e-6
ROUTE_SCALE = 2.5
TILE = 256
PITCH = TILE + 4
GROUP = 4
RING = 4
ORDER = (("D", 0), ("S", 5), ("D", 1), ("S", 5), ("D", 2), ("S", 5), ("D", 3), ("S", 5), ("G", 0), ("S", 6), ("U", 0), ("S", 5), ("G", 1), ("S", 5), ("U", 1), ("S", 5), ("G", 2), ("S", 6), ("U", 2), ("S", 5), ("G", 3), ("S", 6), ("U", 3), ("S", 6), ("H", 0))
LANES = 128
PLAN = (("S", 3), ("P", 2), ("S", 2), ("S", 1))
CHUNKS = tuple(size for _, size in PLAN)
VMEM_LIMIT = 60 * 1024 * 1024


def rms_norm(vals, gain):
    vals = vals.astype(jnp.float32)
    scaled = vals * lax.rsqrt(jnp.mean(vals * vals, axis=-1, keepdims=True) + EPS)
    return (scaled * gain).astype(jnp.bfloat16)


def mm(lhs, rhs):
    return jnp.dot(lhs, rhs, preferred_element_type=jnp.float32)


def swiglu(rows, w_gate, w_up, w_down):
    hidden = (jax.nn.silu(mm(rows, w_gate)) * mm(rows, w_up)).astype(jnp.bfloat16)
    return mm(hidden, w_down).astype(jnp.bfloat16)


def to_blocks(shard):
    rows, cols = shard.shape
    return shard.reshape(rows, cols // LANES, LANES).transpose(1, 0, 2).reshape(-1, LANES)


def from_blocks(gathered, start, rows, cols):
    groups = gathered.shape[0]
    blocks = cols // LANES
    part = gathered[:, start : start + rows * blocks].reshape(groups, blocks, rows, LANES)
    return part.transpose(0, 2, 1, 3).reshape(groups * rows, cols)


def attn_kernel(scale, block, qn_ref, qp_ref, qs_ref, kn_ref, kr_ref, v_ref, cos_ref, sin_ref, o_ref):
    seq = qn_ref.shape[0]
    keys = jnp.concatenate([kn_ref[...], kr_ref[...]], axis=1)
    vals = v_ref[...]
    for start in range(0, seq, block):
        stop = start + block
        turned = qp_ref[start:stop, :].astype(jnp.float32) * cos_ref[start:stop, :] + qs_ref[start:stop, :].astype(jnp.float32) * sin_ref[start:stop, :]
        query = jnp.concatenate([qn_ref[start:stop, :], turned.astype(jnp.bfloat16)], axis=1)
        scores = lax.dot_general(query, keys[:stop], (((1,), (1,)), ((), ())), preferred_element_type=jnp.float32)
        row = lax.broadcasted_iota(jnp.int32, scores.shape, 0) + start
        col = lax.broadcasted_iota(jnp.int32, scores.shape, 1)
        scores = jnp.where(row >= col, scores * scale, -jnp.inf)
        expo = jnp.exp(scores - jnp.max(scores, axis=1, keepdims=True))
        probs = (expo * (1.0 / jnp.sum(expo, axis=1, keepdims=True))).astype(jnp.bfloat16)
        o_ref[start:stop, :] = mm(probs, vals[:stop]).astype(jnp.bfloat16)


def attention_core(q_nope, q_pe, k_nope, k_rot, values, cos_w, sin_w, seq_len, scale):
    tokens, width = q_nope.shape
    seqs, heads = tokens // seq_len, width // LANES
    spec = lambda fn: pl.BlockSpec((seq_len, LANES), fn)
    return pl.pallas_call(
        functools.partial(attn_kernel, scale, 256),
        grid=(seqs, heads),
        in_specs=[
            spec(lambda s, h: (s, h)),
            spec(lambda s, h: (s, h // 2)),
            spec(lambda s, h: (s, heads // 2 + h // 2)),
            spec(lambda s, h: (s, h)),
            spec(lambda s, h: (s, h % 2)),
            spec(lambda s, h: (s, h)),
            spec(lambda s, h: (0, 0)),
            spec(lambda s, h: (0, 0)),
        ],
        out_specs=spec(lambda s, h: (s, h)),
        out_shape=jax.ShapeDtypeStruct((tokens, width), jnp.bfloat16),
        cost_estimate=pl.CostEstimate(flops=4 * tokens * seq_len * width, bytes_accessed=10 * tokens * width, transcendentals=0),
        name="attention_core",
    )(q_nope, q_pe, q_pe, k_nope, k_rot, values, cos_w, sin_w)


def swap_halves(cols, half):
    rows, width = cols.shape
    pairs = cols.reshape(rows, width // (2 * half), 2, half)
    return pairs[:, :, ::-1, :].reshape(rows, width)


def attention(normed, w_dq, g_q, w_uq, w_dkv, g_kv, w_uk, w_uv, w_out, seq_len, rope_dim):
    tokens = normed.shape[0]
    num_seqs = tokens // seq_len
    kv_rank, heads_nope = w_uk.shape
    half = rope_dim // 2
    heads = (w_uq.shape[1] - heads_nope) // rope_dim
    nope_dim = heads_nope // heads
    positions = jnp.arange(seq_len)
    inv_freq = 1.0 / (ROPE_BASE ** (jnp.arange(0, rope_dim, 2).astype(jnp.float32) / rope_dim))
    angles = positions.astype(jnp.float32)[:, None] * inv_freq[None, :]
    cos_t, sin_t = jnp.cos(angles), jnp.sin(angles)
    cos_w = jnp.concatenate([cos_t] * 4, axis=1)
    sin_w = jnp.concatenate([-sin_t, sin_t] * 2, axis=1)
    q_lat = rms_norm(mm(normed, w_dq).astype(jnp.bfloat16), g_q)
    q_nope = mm(q_lat, w_uq[:, :heads_nope]).astype(jnp.bfloat16)
    w_pe = w_uq[:, heads_nope:]
    q_pe = mm(q_lat, jnp.concatenate([w_pe, swap_halves(w_pe, half)], axis=1)).astype(jnp.bfloat16)

    kv_all = mm(normed, w_dkv).astype(jnp.bfloat16)
    latent = rms_norm(kv_all[:, :kv_rank], g_kv)
    k_pe = kv_all[:, kv_rank:].reshape(num_seqs, seq_len, 2 * rope_dim).astype(jnp.float32)
    k_rot = k_pe[..., :rope_dim] * cos_w[None, :, :rope_dim] + k_pe[..., rope_dim:] * sin_w[None, :, :rope_dim]
    k_rot = k_rot.astype(jnp.bfloat16).reshape(tokens, rope_dim)
    blank = jnp.zeros_like(k_rot)
    k_rot = jnp.concatenate([k_rot, blank, blank, k_rot], axis=1)
    k_nope = mm(latent, w_uk).astype(jnp.bfloat16)
    values = mm(latent, w_uv).astype(jnp.bfloat16)
    attended = attention_core(q_nope, q_pe, k_nope, k_rot, values, cos_w, sin_w, seq_len, (nope_dim + rope_dim) ** -0.5)
    return mm(attended, w_out).astype(jnp.bfloat16)


def moe_kernel(first, last, arrays, meta_ref, rank_ref, gate_ref, tab_hbm, u_hbm, *refs):
    if first:
        h_hbm, s_hbm, *refs = refs
    else:
        a_hbm, *refs = refs
    w_hbms, refs = refs[:arrays], refs[arrays:]
    o_hbm, u_vm, acc, wbuf, *refs = refs
    x_bufs, o_bufs, h_bufs = refs[0:2], refs[2:4], refs[4:6]
    t_next, t_prev, s_prev = refs[6 : 6 + RING], refs[6 + RING : 6 + 2 * RING], refs[6 + 2 * RING : 6 + 3 * RING]
    st_a, st_b, wsem, sem_a, sem_b, asem, lsem = refs[6 + 3 * RING :]
    tokens, width = u_hbm.shape
    pieces = width // LANES
    inter = w_hbms[0].shape[2]
    tile_lo, tile_hi, experts = meta_ref[0], meta_ref[1], meta_ref[2]
    blocks = tokens // TILE

    def w_start(order):
        slot = lax.rem(order, 3)
        name = meta_ref[3 + order]
        low = 0
        for w_hbm in w_hbms:
            size = w_hbm.shape[0]

            @pl.when((name >= low) & (name < low + size))
            def _(w_hbm=w_hbm, low=low):
                pltpu.make_async_copy(w_hbm.at[name - low], wbuf.at[slot], wsem.at[slot]).start()

            low += size

    def w_wait(order):
        slot = lax.rem(order, 3)
        pltpu.make_async_copy(w_hbms[0].at[0], wbuf.at[slot], wsem.at[slot]).wait()

    @pl.when(experts > 0)
    def _():
        w_start(0)

    if not first:
        acc_in = pltpu.make_async_copy(a_hbm, acc.at[pl.ds(0, tokens * pieces), :], asem)
        acc_in.start()

    def spread(dst, base, block):
        for j in range(pieces):
            dst[pl.ds(base * pieces + j, TILE, stride=pieces), :] = block[:, j * LANES : (j + 1) * LANES]

    def load_rows(src, stage, sem, step):
        return pltpu.make_async_copy(src.at[pl.ds(step * TILE, TILE), :], stage.at[lax.rem(step, 2)], sem.at[lax.rem(step, 2)])

    load_rows(u_hbm, st_a, sem_a, 0).start()

    @pl.loop(0, blocks)
    def _(step):
        @pl.when(step + 1 < blocks)
        def _():
            load_rows(u_hbm, st_a, sem_a, step + 1).start()

        load_rows(u_hbm, st_a, sem_a, step).wait()
        spread(u_vm, step * TILE, st_a[lax.rem(step, 2)].astype(jnp.float32))

    u_vm[pl.ds(tokens * pieces, 8), :] = jnp.zeros((8, LANES), jnp.float32)
    if first:
        load_rows(h_hbm, st_a, sem_a, 0).start()
        load_rows(s_hbm, st_b, sem_b, 0).start()

        @pl.loop(0, blocks)
        def _(step):
            @pl.when(step + 1 < blocks)
            def _():
                load_rows(h_hbm, st_a, sem_a, step + 1).start()
                load_rows(s_hbm, st_b, sem_b, step + 1).start()

            load_rows(h_hbm, st_a, sem_a, step).wait()
            load_rows(s_hbm, st_b, sem_b, step).wait()
            slot = lax.rem(step, 2)
            spread(acc, step * TILE, st_a[slot].astype(jnp.float32) + st_b[slot].astype(jnp.float32))
    else:
        acc_in.wait()
    acc[pl.ds(tokens * pieces, 8), :] = jnp.zeros((8, LANES), jnp.float32)

    idle = tab_hbm.shape[0] - 1
    count = tile_hi - tile_lo

    def tile_at(step):
        return jnp.where((step >= 0) & (step < count), tile_lo + step, idle)

    def list_copies(step, turn):
        ahead, behind = tab_hbm.at[tile_at(step + 1)], tab_hbm.at[tile_at(step - 2)]
        return (
            pltpu.make_async_copy(ahead.at[0], t_next[turn], lsem.at[turn, 0]),
            pltpu.make_async_copy(behind.at[0], t_prev[turn], lsem.at[turn, 1]),
            pltpu.make_async_copy(behind.at[1], s_prev[turn], lsem.at[turn, 2]),
        )

    def row_at(offset):
        return pl.ds(pl.multiple_of(offset, pieces), pieces)

    def order_at(step):
        return jnp.where((step >= 0) & (step < count), rank_ref[tile_at(step)], 0)

    depth = 2 * LANES
    half = TILE // 2

    def column(buf, j):
        parts = [buf[pl.ds(j * PITCH + odd, half, stride=2), :] for odd in (0, 1)]
        return jnp.concatenate(parts, axis=0)

    def tile_step(step, turn):
        parity = turn % 2
        x_now, x_next = x_bufs[parity], x_bufs[1 - parity]
        h_now, h_prev = h_bufs[parity], h_bufs[1 - parity]
        o_now, o_prev = o_bufs[parity], o_bufs[1 - parity]
        ahead, behind, slots = t_next[turn], t_prev[turn], s_prev[turn]
        for copy in list_copies(step + RING - 1, (turn + RING - 1) % RING):
            copy.start()
        mine, before = order_at(step), order_at(step - 1)

        @pl.when((step < count) & ((step == 0) | (mine != before)))
        def _():
            w_wait(mine)

            @pl.when(mine + 1 < experts)
            def _():
                w_start(mine + 1)

        for copy in list_copies(step, turn):
            copy.wait()

        def side_work(low, high):
            for start in range(low, high, GROUP):
                for r in range(start, start + GROUP):
                    x_next[pl.ds(r, pieces, stride=PITCH), :] = u_vm[row_at(ahead[r]), :]
                spots = [behind[r] for r in range(start, start + GROUP)]
                sums = [acc[row_at(t), :] + gate_ref[slots[start + r]] * o_prev[pl.ds(start + r, pieces, stride=PITCH), :] for r, t in enumerate(spots)]
                for r, total in enumerate(sums):
                    acc[row_at(behind[start + r]), :] = total

        w_now, w_prev = wbuf.at[lax.rem(mine, 3)], wbuf.at[lax.rem(before, 3)]
        sums, parts = {}, {}
        done = 0
        for kind, k in ORDER:
            if kind in "GU":
                if k not in parts:
                    parts[k] = jnp.concatenate([column(x_now, 2 * k).astype(jnp.bfloat16), column(x_now, 2 * k + 1).astype(jnp.bfloat16)], axis=1)
                low = (0 if kind == "G" else width) + k * depth
                term = mm(parts[k], w_now[low : low + depth, :])
                sums[kind] = term if k == 0 else sums[kind] + term
            elif kind == "D":
                low = 2 * width + k * inter
                out = mm(h_prev[...], w_prev[low : low + inter, :]).astype(jnp.bfloat16).astype(jnp.float32)
                for j in range(inter // LANES):
                    for odd in (0, 1):
                        at = pl.ds((k * (inter // LANES) + j) * PITCH + odd, half, stride=2)
                        o_now[at, :] = out[odd * half : (odd + 1) * half, j * LANES : (j + 1) * LANES]
            elif kind == "S":
                side_work(done, done + k * GROUP)
                done += k * GROUP
            else:
                h_now[...] = (jax.nn.silu(sums["G"]) * sums["U"]).astype(jnp.bfloat16)
        side_work(done, TILE)

    first_list = pltpu.make_async_copy(tab_hbm.at[tile_at(0), 0], t_next[RING - 1], lsem.at[RING - 1, 0])
    first_list.start()
    for ahead in range(RING - 1):
        for copy in list_copies(ahead, ahead):
            copy.start()
    first_list.wait()
    for r in range(TILE):
        x_bufs[0][pl.ds(r, pieces, stride=PITCH), :] = u_vm[row_at(t_next[RING - 1][r]), :]

    rounds = (count + RING + 1) // RING

    @pl.loop(0, rounds)
    def _(i):
        for turn in range(RING):
            tile_step(RING * i + turn, turn)

    for ahead in range(RING - 1):
        for copy in list_copies(RING * rounds + ahead, ahead):
            copy.wait()

    if last:

        def store_rows(step):
            return pltpu.make_async_copy(st_a.at[lax.rem(step, 2)], o_hbm.at[pl.ds(step * TILE, TILE), :], sem_a.at[lax.rem(step, 2)])

        @pl.loop(0, blocks)
        def _(step):
            @pl.when(step >= 2)
            def _():
                store_rows(step - 2).wait()

            parts = [acc[pl.ds(step * TILE * pieces + j, TILE, stride=pieces), :].astype(jnp.bfloat16) for j in range(pieces)]
            st_a[lax.rem(step, 2)] = jnp.concatenate(parts, axis=1)
            store_rows(step).start()

        store_rows(blocks - 2).wait()
        store_rows(blocks - 1).wait()
    else:
        acc_out = pltpu.make_async_copy(acc.at[pl.ds(0, tokens * pieces), :], o_hbm, asem)
        acc_out.start()
        acc_out.wait()


def moe_call(first, last, meta, table, ranks, gates, u_norm, extra, weights):
    tokens, width = u_norm.shape
    pieces = width // LANES
    experts = sum(w.shape[0] for w in weights)
    wrows, inter = weights[0].shape[1:]
    smem = pl.BlockSpec(memory_space=pltpu.SMEM)
    hbm = pl.BlockSpec(memory_space=pl.ANY)
    scratch = [
        pltpu.VMEM((tokens * pieces + 8, LANES), jnp.float32),
        pltpu.VMEM((tokens * pieces + 8, LANES), jnp.float32),
        pltpu.VMEM((3, wrows, inter), jnp.bfloat16),
        *[pltpu.VMEM((pieces * PITCH, LANES), jnp.float32)] * 4,
        *[pltpu.VMEM((TILE, inter), jnp.bfloat16)] * 2,
        *[pltpu.SMEM((TILE,), jnp.int32)] * (3 * RING),
        pltpu.VMEM((2, TILE, width), jnp.bfloat16),
        pltpu.VMEM((2, TILE, width), jnp.bfloat16),
        pltpu.SemaphoreType.DMA((3,)),
        pltpu.SemaphoreType.DMA((2,)),
        pltpu.SemaphoreType.DMA((2,)),
        pltpu.SemaphoreType.DMA,
        pltpu.SemaphoreType.DMA((RING, 3)),
    ]
    out_shape = jax.ShapeDtypeStruct((tokens, width), jnp.bfloat16) if last else jax.ShapeDtypeStruct((tokens * pieces, LANES), jnp.float32)
    rows = experts * tokens // 8
    return pl.pallas_call(
        functools.partial(moe_kernel, first, last, len(weights)),
        in_specs=[smem] * 3 + [hbm] * (2 + len(extra) + len(weights)),
        out_specs=hbm,
        out_shape=out_shape,
        scratch_shapes=scratch,
        compiler_params=pltpu.CompilerParams(vmem_limit_bytes=VMEM_LIMIT),
        cost_estimate=pl.CostEstimate(flops=2 * rows * wrows * inter, bytes_accessed=2 * experts * wrows * inter, transcendentals=0),
        name="routed_experts",
    )(meta, ranks, gates, table, u_norm, *extra, *weights)


def route_plan(choice_ids, num_experts, groups, here):
    tokens, num_top = choice_ids.shape
    local = num_experts // groups
    device, index = choice_ids // local, choice_ids % local
    rank = jnp.zeros_like(choice_ids)
    low = 0
    for way, size in PLAN:
        place = device ^ here if way == "P" else device
        rank = jnp.where((index >= low) & (index < low + size), low * groups + place * size + index - low, rank)
        low += size
    hits = rank[:, :, None] == jnp.arange(num_experts)[None, None, :]
    counts = jnp.sum(hits.astype(jnp.int32), axis=(0, 1))
    slots = jnp.arange(tokens)[:, None] * num_top + jnp.arange(num_top)[None, :]
    keys = (rank * 65536 + slots).reshape(-1)
    spare = jnp.arange(TILE)[None, :] < ((-counts) % TILE)[:, None]
    dummy = tokens * num_top
    fill = jnp.where(spare, jnp.arange(num_experts)[:, None] * 65536 + dummy, num_experts * 65536 + dummy)
    ordered = jnp.sort(jnp.concatenate([keys, fill.reshape(-1)]), stable=False)
    tiles = (counts + TILE - 1) // TILE
    spans = [(sum(CHUNKS[:i]) * groups, sum(CHUNKS[: i + 1]) * groups) for i in range(len(CHUNKS))]
    experts = jnp.arange(num_experts)
    chunk = sum((experts >= low).astype(jnp.int32) for low, _ in spans) - 1
    used = counts > 0
    ahead = (chunk[:, None] == chunk[None, :]) & (experts[None, :] < experts[:, None])
    order = jnp.sum(jnp.where(ahead & used[None, :], 1, 0), axis=1)
    start = jnp.array([low for low, _ in spans])
    stop = jnp.array([high for _, high in spans])
    member = (experts[None, :] >= start[:, None]) & (experts[None, :] < stop[:, None]) & used[None, :]
    names = jnp.sum(jnp.where(member[:, None, :] & (order[None, None, :] == experts[None, :, None]), experts[None, None, :] - start[:, None, None], 0), axis=2)
    first = jnp.sum(jnp.where(experts[None, :] < start[:, None], tiles[None, :], 0), axis=1)
    final = jnp.sum(jnp.where(experts[None, :] < stop[:, None], tiles[None, :], 0), axis=1)
    metas = jnp.concatenate([jnp.stack([first, final, jnp.sum(member.astype(jnp.int32), axis=1)], axis=1), names], axis=1).astype(jnp.int32)
    ranks = ordered[::TILE] // 65536
    orders = jnp.sum(jnp.where(ranks[:, None] == experts[None, :], order[None, :], 0), axis=1)
    low = ordered & 65535
    table = jnp.stack([(low & ~7).reshape(-1, TILE), low.reshape(-1, TILE)], axis=1)
    return table, orders, metas


def after(vals, token):
    return lax.optimization_barrier((vals, token))[0]


def spread_pair(own, early, late):
    count = lax.axis_size(AXIS)

    def send(bit, vals):
        return lax.ppermute(vals, AXIS, [(i, i ^ bit) for i in range(count)])

    own = after(own, early)
    along_x, along_y = after((send(2, own), send(4, own)), late)
    far = send(4, along_x[:1]), send(2, along_y[1:])
    own_core = [own, along_x, along_y, *far]
    other = [send(1, vals) for vals in own_core]
    return (own, other[0], along_x, other[1], along_y, other[2], *far, *other[3:])


def solution(mesh):
    groups = mesh.shape[AXIS]
    rows_spec = P(AXIS, None)
    vec_spec = P(AXIS)
    full_spec = P(None, None)
    cube_spec = P(AXIS, None, None)
    in_specs = (cube_spec, vec_spec, rows_spec, rows_spec, rows_spec, vec_spec, rows_spec, vec_spec, rows_spec, rows_spec, vec_spec, rows_spec, rows_spec, rows_spec, vec_spec, full_spec, cube_spec, cube_spec, cube_spec, full_spec, full_spec, full_spec, cube_spec)

    def gather(shard):
        return lax.all_gather(shard, AXIS, axis=0, tiled=True)

    def local(x_resid, g_mlp, w_gate, w_up, w_down, g_attn, w_dq, g_q, w_uq, w_dkv, g_kv, w_uk, w_uv, w_out, g_moe, w_router, we_gate, we_up, we_down, ws_gate, ws_up, ws_down, expert_ids):
        num_seqs, seq_len, width = x_resid.shape
        tokens = num_seqs * seq_len
        num_experts = w_router.shape[0]
        inter = we_gate.shape[2]
        flat_x = x_resid.reshape(tokens, width)
        choice_ids = expert_ids.reshape(tokens, expert_ids.shape[2])

        gains = [g_mlp, g_attn, g_q, g_kv, g_moe]
        sizes = [g.shape[0] for g in gains]
        packed = lax.all_gather(jnp.concatenate(gains), AXIS, axis=0, tiled=False)
        offs = [sum(sizes[:i]) for i in range(len(sizes))]
        g_mlp, g_attn, g_q, g_kv, g_moe = [packed[:, o : o + s].reshape(-1) for o, s in zip(offs, sizes)]

        inner = w_gate.shape[1]
        gate_up = gather(jnp.concatenate([w_gate, w_up], axis=1))
        kv_rank = w_uk.shape[0] * groups
        rope_dim = w_dkv.shape[1] - kv_rank
        heads = (w_uq.shape[1] - w_uk.shape[1]) // rope_dim
        nope_dim = w_uk.shape[1] // heads
        per_head = w_uq.reshape(w_uq.shape[0], heads, nope_dim + rope_dim)
        uq_local = jnp.concatenate([per_head[:, :, :nope_dim].reshape(-1, heads * nope_dim), per_head[:, :, nope_dim:].reshape(-1, heads * rope_dim)], axis=1)
        dkv_local = jnp.concatenate([w_dkv, swap_halves(w_dkv[:, kv_rank:], rope_dim // 2)], axis=1)
        shards = [w_down, w_dq, dkv_local, uq_local, w_uk, w_uv, w_out]
        blocks = [to_blocks(s) for s in shards]
        attn_w = gather(jnp.concatenate(blocks, axis=0)[None])
        starts = [sum(b.shape[0] for b in blocks[:i]) for i in range(len(blocks))]
        down, w_dq, w_dkv, w_uq, w_uk, w_uv, w_out = [from_blocks(attn_w, st, s.shape[0], s.shape[1]) for st, s in zip(starts, shards)]

        down_blocks = we_down.reshape(we_down.shape[0], inter, width // inter, inter).transpose(0, 2, 1, 3).reshape(we_down.shape[0], width, inter)
        pack = jnp.concatenate([we_gate, we_up, down_blocks], axis=1)
        table, ranks, metas = route_plan(choice_ids, num_experts, groups, lax.axis_index(AXIS))

        normed = rms_norm(flat_x, g_mlp)
        hidden = (jax.nn.silu(mm(normed, gate_up[:, :inner])) * mm(normed, gate_up[:, inner:])).astype(jnp.bfloat16)
        mlp_out = mm(hidden, down).astype(jnp.bfloat16)
        h_one = (flat_x.astype(jnp.float32) + mlp_out.astype(jnp.float32)).astype(jnp.bfloat16)
        expert_w = []
        low = 0
        for way, size in PLAN:
            part = pack[low : low + size]
            expert_w.append(spread_pair(part, gate_up, h_one) if way == "P" else (gather(part),))
            low += size

        attn_out = attention(rms_norm(h_one, g_attn), w_dq, g_q, w_uq, w_dkv, g_kv, w_uk, w_uv, w_out, seq_len, rope_dim)
        h_two = (h_one.astype(jnp.float32) + attn_out.astype(jnp.float32)).astype(jnp.bfloat16)
        u_norm = rms_norm(h_two, g_moe)
        logits = jnp.einsum("td,ed->te", u_norm.astype(jnp.float32), w_router, precision=lax.Precision.HIGHEST)
        scores = jax.nn.sigmoid(logits)
        hits = choice_ids[:, :, None] == jnp.arange(num_experts)[None, None, :]
        picked = jnp.sum(jnp.where(hits, scores[:, None, :], 0.0), axis=2)
        gates = (ROUTE_SCALE * picked / jnp.sum(picked, axis=1, keepdims=True)).reshape(-1)
        gates = jnp.concatenate([gates, jnp.zeros((8,), jnp.float32)])
        shared = swiglu(u_norm, ws_gate, ws_up, ws_down)

        total = None
        for i, weights in enumerate(expert_w):
            extra = (h_two, shared) if i == 0 else (total,)
            total = moe_call(i == 0, i == len(expert_w) - 1, metas[i], table, ranks, gates, u_norm, extra, weights)
        return total.reshape(num_seqs, seq_len, width)

    return jax.shard_map(local, mesh=mesh, in_specs=in_specs, out_specs=cube_spec, check_vma=False)
```

```python
import functools

import jax
import jax.numpy as jnp
from jax import lax
from jax.experimental import pallas as pl
from jax.experimental.pallas import tpu as pltpu
from jax.sharding import PartitionSpec as P


AXIS = "fsdp"
ROPE_BASE = 10000.0
EPS = 1e-6
ROUTE_SCALE = 2.5
TILE = 256
PITCH = TILE + 4
GROUP = 4
RING = 4
STAGES = 6
FF_STEP = 256
DENSE_ROWS = 512
PREP_ROWS = 512
POST_ROWS = 512
DENSE_LANES = 512
ATTN_LANES = 256
ORDER = (("D", 0), ("S", 5), ("D", 1), ("S", 5), ("D", 2), ("S", 5), ("D", 3), ("S", 5), ("G", 0), ("S", 6), ("U", 0), ("S", 5), ("G", 1), ("S", 5), ("U", 1), ("S", 5), ("G", 2), ("S", 6), ("U", 2), ("S", 5), ("G", 3), ("S", 6), ("U", 3), ("S", 6), ("H", 0))
LANES = 128
PLAN = (("S", 3), ("P", 2), ("S", 2), ("S", 1))
CHUNKS = tuple(size for _, size in PLAN)
VMEM_LIMIT = 60 * 1024 * 1024


def rms_rows(vals, gain):
    scaled = vals * lax.rsqrt(jnp.mean(vals * vals, axis=-1, keepdims=True) + EPS)
    return (scaled * gain).astype(jnp.bfloat16)


def mm(lhs, rhs):
    return jnp.dot(lhs, rhs, preferred_element_type=jnp.float32)


def to_blocks(shard, lanes):
    rows, cols = shard.shape
    return shard.reshape(rows, cols // lanes, lanes).transpose(1, 0, 2).reshape(-1, lanes)


def load_weights(packed, starts, dsts, sems):
    groups, _, lanes = packed.shape
    for start, dst, sem in zip(starts, dsts, sems):
        rows = dst.shape[0] // groups
        for b in range(dst.shape[1] // lanes):
            for d in range(groups):
                src = packed.at[d, pl.ds(start + b * rows, rows), :]
                pltpu.make_async_copy(src, dst.at[pl.ds(d * rows, rows), pl.ds(b * lanes, lanes)], sem).start()


def await_weights(dst, sem):
    pltpu.make_async_copy(dst, dst, sem).wait()


def dense_kernel(starts, packed, gain_ref, x_ref, o_ref, w_in, w_out, hid, sems):
    first = pl.program_id(0) == 0

    @pl.when(first)
    def _():
        load_weights(packed, starts, (w_in, w_out), (sems.at[0], sems.at[1]))

    rows = rms_rows(x_ref[...].astype(jnp.float32), gain_ref[...])

    @pl.when(first)
    def _():
        await_weights(w_in, sems.at[0])
        await_weights(w_out, sems.at[1])

    inner = hid.shape[1]
    for c in range(0, inner, FF_STEP):
        gate = mm(rows, w_in[:, c : c + FF_STEP])
        upper = mm(rows, w_in[:, inner + c : inner + c + FF_STEP])
        hid[:, c : c + FF_STEP] = (jax.nn.silu(gate) * upper).astype(jnp.bfloat16)
    for c in range(0, o_ref.shape[1], FF_STEP):
        out = mm(hid[...], w_out[:, c : c + FF_STEP]).astype(jnp.bfloat16)
        o_ref[:, c : c + FF_STEP] = (x_ref[:, c : c + FF_STEP].astype(jnp.float32) + out.astype(jnp.float32)).astype(jnp.bfloat16)


def dense_layer(packed, starts, flat_x, gain, inner):
    tokens, width = flat_x.shape
    block = pl.BlockSpec((DENSE_ROWS, width), lambda i: (i, 0))
    return pl.pallas_call(
        functools.partial(dense_kernel, starts),
        grid=(tokens // DENSE_ROWS,),
        in_specs=[pl.BlockSpec(memory_space=pl.ANY), pl.BlockSpec((1, width), lambda i: (0, 0)), block],
        out_specs=block,
        out_shape=jax.ShapeDtypeStruct((tokens, width), jnp.bfloat16),
        scratch_shapes=[
            pltpu.VMEM((width, 2 * inner), jnp.bfloat16),
            pltpu.VMEM((inner, width), jnp.bfloat16),
            pltpu.VMEM((DENSE_ROWS, inner), jnp.bfloat16),
            pltpu.SemaphoreType.DMA((2,)),
        ],
        compiler_params=pltpu.CompilerParams(vmem_limit_bytes=VMEM_LIMIT),
        cost_estimate=pl.CostEstimate(flops=6 * tokens * width * inner, bytes_accessed=4 * tokens * width + 6 * width * inner, transcendentals=0),
        name="dense_layer",
    )(packed, gain.reshape(1, width), flat_x)


def attn_kernel(scale, block, qn_ref, qr_ref, kn_ref, kr_ref, v_ref, o_ref):
    seq = qn_ref.shape[0]
    keys = jnp.concatenate([kn_ref[...], kr_ref[...]], axis=1)
    vals = v_ref[...]
    for start in range(0, seq, block):
        stop = start + block
        query = jnp.concatenate([qn_ref[start:stop, :], qr_ref[start:stop, :]], axis=1)
        scores = lax.dot_general(query, keys[:stop], (((1,), (1,)), ((), ())), preferred_element_type=jnp.float32)
        row = lax.broadcasted_iota(jnp.int32, scores.shape, 0) + start
        col = lax.broadcasted_iota(jnp.int32, scores.shape, 1)
        scores = jnp.where(row >= col, scores * scale, -jnp.inf)
        expo = jnp.exp(scores - jnp.max(scores, axis=1, keepdims=True))
        probs = (expo * (1.0 / jnp.sum(expo, axis=1, keepdims=True))).astype(jnp.bfloat16)
        o_ref[start:stop, :] = mm(probs, vals[:stop]).astype(jnp.bfloat16)


def attention_core(q_nope, q_rot, k_nope, k_rot, values, seq_len, scale):
    tokens, width = q_nope.shape
    seqs, heads = tokens // seq_len, width // LANES
    spec = lambda fn: pl.BlockSpec((seq_len, LANES), fn)
    return pl.pallas_call(
        functools.partial(attn_kernel, scale, 256),
        grid=(seqs, heads),
        in_specs=[
            spec(lambda s, h: (s, h)),
            spec(lambda s, h: (s, h // 2)),
            spec(lambda s, h: (s, h)),
            spec(lambda s, h: (s, h % 2)),
            spec(lambda s, h: (s, h)),
        ],
        out_specs=spec(lambda s, h: (s, h)),
        out_shape=jax.ShapeDtypeStruct((tokens, width), jnp.bfloat16),
        cost_estimate=pl.CostEstimate(flops=4 * tokens * seq_len * width, bytes_accessed=10 * tokens * width, transcendentals=0),
        name="attention_core",
    )(q_nope, q_rot, k_nope, k_rot, values)


def prep_kernel(starts, packed, ga_ref, gq_ref, gkv_ref, cos_ref, sin_ref, h_ref, qn_ref, qr_ref, kn_ref, kr_ref, v_ref, w_low, w_q, w_k, w_v, sems):
    first = pl.program_id(0) == 0
    weights = (w_low, w_q, w_k, w_v)

    @pl.when(first)
    def _():
        load_weights(packed, starts, weights, [sems.at[i] for i in range(4)])

    rows = rms_rows(h_ref[...].astype(jnp.float32), ga_ref[...])

    @pl.when(first)
    def _():
        for i, dst in enumerate(weights):
            await_weights(dst, sems.at[i])

    lane = lax.broadcasted_iota(jnp.int32, (h_ref.shape[0], LANES), 1)

    def turn(vals):
        swapped = jnp.where(lane % 64 < 32, pltpu.roll(vals, LANES - 32, 1), pltpu.roll(vals, 32, 1))
        return (vals * cos_ref[...] + swapped * sin_ref[...]).astype(jnp.bfloat16)

    q_rank, kv_rank, nope = w_q.shape[0], w_k.shape[0], w_k.shape[1]
    low = mm(rows, w_low[...]).astype(jnp.bfloat16).astype(jnp.float32)
    q_lat = rms_rows(low[:, :q_rank], gq_ref[...])
    latent = rms_rows(low[:, q_rank : q_rank + kv_rank], gkv_ref[...])
    for c in range(0, nope, FF_STEP):
        kn_ref[:, c : c + FF_STEP] = mm(latent, w_k[:, c : c + FF_STEP]).astype(jnp.bfloat16)
        v_ref[:, c : c + FF_STEP] = mm(latent, w_v[:, c : c + FF_STEP]).astype(jnp.bfloat16)
        qn_ref[:, c : c + FF_STEP] = mm(q_lat, w_q[:, c : c + FF_STEP]).astype(jnp.bfloat16)
    for c in range(nope, w_q.shape[1], FF_STEP):
        part = mm(q_lat, w_q[:, c : c + FF_STEP]).astype(jnp.bfloat16).astype(jnp.float32)
        for j in range(0, FF_STEP, LANES):
            qr_ref[:, c - nope + j : c - nope + j + LANES] = turn(part[:, j : j + LANES])
    key = turn(low[:, q_rank + kv_rank :]).astype(jnp.float32)
    kr_ref[:, 0:LANES] = jnp.where(lane < 64, key, 0.0).astype(jnp.bfloat16)
    kr_ref[:, LANES : 2 * LANES] = jnp.where(lane < 64, 0.0, key).astype(jnp.bfloat16)


def attention_prep(packed, starts, h_one, g_attn, g_q, g_kv, cos_w, sin_w, nope, pe):
    tokens, width = h_one.shape
    seq_blocks = cos_w.shape[0] // PREP_ROWS
    q_rank, kv_rank = g_q.shape[0], g_kv.shape[0]
    vec = lambda n: pl.BlockSpec((1, n), lambda i: (0, 0))
    rows = lambda n: pl.BlockSpec((PREP_ROWS, n), lambda i: (i, 0))
    table = pl.BlockSpec((PREP_ROWS, LANES), lambda i: (i % seq_blocks, 0))
    cols = (nope, pe, nope, 2 * LANES, nope)
    return pl.pallas_call(
        functools.partial(prep_kernel, starts),
        grid=(tokens // PREP_ROWS,),
        in_specs=[pl.BlockSpec(memory_space=pl.ANY), vec(width), vec(q_rank), vec(kv_rank), table, table, rows(width)],
        out_specs=[rows(n) for n in cols],
        out_shape=[jax.ShapeDtypeStruct((tokens, n), jnp.bfloat16) for n in cols],
        scratch_shapes=[
            pltpu.VMEM((width, q_rank + kv_rank + LANES), jnp.bfloat16),
            pltpu.VMEM((q_rank, nope + pe), jnp.bfloat16),
            pltpu.VMEM((kv_rank, nope), jnp.bfloat16),
            pltpu.VMEM((kv_rank, nope), jnp.bfloat16),
            pltpu.SemaphoreType.DMA((4,)),
        ],
        compiler_params=pltpu.CompilerParams(vmem_limit_bytes=VMEM_LIMIT),
        cost_estimate=pl.CostEstimate(flops=2 * tokens * (width * 768 + q_rank * (nope + pe) + 2 * kv_rank * nope), bytes_accessed=12 * tokens * width, transcendentals=0),
        name="attention_prep",
    )(packed, g_attn.reshape(1, -1), g_q.reshape(1, -1), g_kv.reshape(1, -1), cos_w, sin_w, h_one)


def post_kernel(starts, packed, gain_ref, wr_ref, wsi_ref, wso_ref, att_ref, h_ref, u_ref, s_ref, o_ref, w_out, sems):
    first = pl.program_id(0) == 0

    @pl.when(first)
    def _():
        load_weights(packed, starts, (w_out,), (sems.at[0],))
        await_weights(w_out, sems.at[0])

    count, width = h_ref.shape
    pieces = width // LANES
    attn = mm(att_ref[...], w_out[...]).astype(jnp.bfloat16)
    h_two = (h_ref[...].astype(jnp.float32) + attn.astype(jnp.float32)).astype(jnp.bfloat16).astype(jnp.float32)
    rows = rms_rows(h_two, gain_ref[...])
    u_ref[...] = rows
    terms = lax.dot_general(rows, wr_ref[...], (((1,), (1,)), ((), ())), preferred_element_type=jnp.float32)
    logits = terms[:, :LANES] + pltpu.roll(terms[:, :LANES], LANES // 2, 1) + terms[:, LANES:]
    s_ref[...] = jax.nn.sigmoid(logits)
    inner = wso_ref.shape[0]
    hidden = (jax.nn.silu(mm(rows, wsi_ref[:, :inner])) * mm(rows, wsi_ref[:, inner:])).astype(jnp.bfloat16)
    shared = mm(hidden, wso_ref[...]).astype(jnp.bfloat16)
    total = h_two + shared.astype(jnp.float32)
    for j in range(pieces):
        o_ref[pl.ds(j, count, stride=pieces), :] = total[:, j * LANES : (j + 1) * LANES]


def attention_post(packed, starts, attended, h_one, gain, wr, ws_in, ws_out):
    tokens, width = h_one.shape
    pieces = width // LANES
    whole = lambda arr: pl.BlockSpec(arr.shape, lambda i: (0, 0))
    rows = lambda n: pl.BlockSpec((POST_ROWS, n), lambda i: (i, 0))
    return pl.pallas_call(
        functools.partial(post_kernel, starts),
        grid=(tokens // POST_ROWS,),
        in_specs=[pl.BlockSpec(memory_space=pl.ANY), pl.BlockSpec((1, width), lambda i: (0, 0)), whole(wr), whole(ws_in), whole(ws_out), rows(width), rows(width)],
        out_specs=[rows(width), rows(LANES), pl.BlockSpec((POST_ROWS * pieces, LANES), lambda i: (i, 0))],
        out_shape=[
            jax.ShapeDtypeStruct((tokens, width), jnp.bfloat16),
            jax.ShapeDtypeStruct((tokens, LANES), jnp.float32),
            jax.ShapeDtypeStruct((tokens * pieces, LANES), jnp.float32),
        ],
        scratch_shapes=[pltpu.VMEM((attended.shape[1], width), jnp.bfloat16), pltpu.SemaphoreType.DMA((1,))],
        compiler_params=pltpu.CompilerParams(vmem_limit_bytes=VMEM_LIMIT),
        cost_estimate=pl.CostEstimate(flops=2 * tokens * width * (width + 1024), bytes_accessed=10 * tokens * width, transcendentals=0),
        name="attention_post",
    )(packed, gain.reshape(1, width), wr, ws_in, ws_out, attended, h_one)


def moe_kernel(last, arrays, meta_ref, rank_ref, gate_ref, tab_hbm, u_hbm, a_hbm, *refs):
    w_hbms, refs = refs[:arrays], refs[arrays:]
    o_hbm, u_vm, acc, wbuf, *refs = refs
    x_bufs, o_bufs, h_bufs = refs[0:2], refs[2:4], refs[4:6]
    t_next, t_prev, s_prev = refs[6 : 6 + RING], refs[6 + RING : 6 + 2 * RING], refs[6 + 2 * RING : 6 + 3 * RING]
    stage, wsem, ssem, asem, lsem = refs[6 + 3 * RING :]
    tokens, width = u_hbm.shape
    pieces = width // LANES
    inter = w_hbms[0].shape[2]
    tile_lo, tile_hi, experts = meta_ref[0], meta_ref[1], meta_ref[2]
    blocks = tokens // TILE

    def w_start(order):
        slot = lax.rem(order, 3)
        name = meta_ref[3 + order]
        low = 0
        for w_hbm in w_hbms:
            size = w_hbm.shape[0]

            @pl.when((name >= low) & (name < low + size))
            def _(w_hbm=w_hbm, low=low):
                pltpu.make_async_copy(w_hbm.at[name - low], wbuf.at[slot], wsem.at[slot]).start()

            low += size

    def w_wait(order):
        slot = lax.rem(order, 3)
        pltpu.make_async_copy(w_hbms[0].at[0], wbuf.at[slot], wsem.at[slot]).wait()

    @pl.when(experts > 0)
    def _():
        w_start(0)

    def row_copy(step):
        slot = lax.rem(step, STAGES)
        return pltpu.make_async_copy(u_hbm.at[pl.ds(step * TILE, TILE), :], stage.at[slot], ssem.at[slot])

    for step in range(min(STAGES - 1, blocks)):
        row_copy(step).start()
    acc_in = pltpu.make_async_copy(a_hbm, acc.at[pl.ds(0, tokens * pieces), :], asem)
    acc_in.start()

    @pl.loop(0, blocks)
    def _(step):
        @pl.when(step + STAGES - 1 < blocks)
        def _():
            row_copy(step + STAGES - 1).start()

        row_copy(step).wait()
        block = stage[lax.rem(step, STAGES)].astype(jnp.float32)
        for j in range(pieces):
            u_vm[pl.ds(step * TILE * pieces + j, TILE, stride=pieces), :] = block[:, j * LANES : (j + 1) * LANES]

    u_vm[pl.ds(tokens * pieces, 8), :] = jnp.zeros((8, LANES), jnp.float32)
    acc[pl.ds(tokens * pieces, 8), :] = jnp.zeros((8, LANES), jnp.float32)

    idle = tab_hbm.shape[0] - 1
    count = tile_hi - tile_lo

    def tile_at(step):
        return jnp.where((step >= 0) & (step < count), tile_lo + step, idle)

    def list_copies(step, turn):
        ahead, behind = tab_hbm.at[tile_at(step + 1)], tab_hbm.at[tile_at(step - 2)]
        return (
            pltpu.make_async_copy(ahead.at[0], t_next[turn], lsem.at[turn, 0]),
            pltpu.make_async_copy(behind.at[0], t_prev[turn], lsem.at[turn, 1]),
            pltpu.make_async_copy(behind.at[1], s_prev[turn], lsem.at[turn, 2]),
        )

    def row_at(offset):
        return pl.ds(pl.multiple_of(offset, pieces), pieces)

    def order_at(step):
        return jnp.where((step >= 0) & (step < count), rank_ref[tile_at(step)], 0)

    depth = 2 * LANES
    half = TILE // 2

    def column(buf, j):
        parts = [buf[pl.ds(j * PITCH + odd, half, stride=2), :] for odd in (0, 1)]
        return jnp.concatenate(parts, axis=0)

    def tile_step(step, turn):
        parity = turn % 2
        x_now, x_next = x_bufs[parity], x_bufs[1 - parity]
        h_now, h_prev = h_bufs[parity], h_bufs[1 - parity]
        o_now, o_prev = o_bufs[parity], o_bufs[1 - parity]
        ahead, behind, slots = t_next[turn], t_prev[turn], s_prev[turn]
        for copy in list_copies(step + RING - 1, (turn + RING - 1) % RING):
            copy.start()
        mine, before = order_at(step), order_at(step - 1)

        @pl.when((step < count) & ((step == 0) | (mine != before)))
        def _():
            w_wait(mine)

            @pl.when(mine + 1 < experts)
            def _():
                w_start(mine + 1)

        for copy in list_copies(step, turn):
            copy.wait()

        def side_work(low, high):
            for start in range(low, high, GROUP):
                for r in range(start, start + GROUP):
                    x_next[pl.ds(r, pieces, stride=PITCH), :] = u_vm[row_at(ahead[r]), :]
                spots = [behind[r] for r in range(start, start + GROUP)]
                sums = [acc[row_at(t), :] + gate_ref[slots[start + r]] * o_prev[pl.ds(start + r, pieces, stride=PITCH), :] for r, t in enumerate(spots)]
                for r, total in enumerate(sums):
                    acc[row_at(behind[start + r]), :] = total

        w_now, w_prev = wbuf.at[lax.rem(mine, 3)], wbuf.at[lax.rem(before, 3)]
        sums, parts = {}, {}
        done = 0
        for kind, k in ORDER:
            if kind in "GU":
                if k not in parts:
                    parts[k] = jnp.concatenate([column(x_now, 2 * k).astype(jnp.bfloat16), column(x_now, 2 * k + 1).astype(jnp.bfloat16)], axis=1)
                low = (0 if kind == "G" else width) + k * depth
                term = mm(parts[k], w_now[low : low + depth, :])
                sums[kind] = term if k == 0 else sums[kind] + term
            elif kind == "D":
                low = 2 * width + k * inter
                out = mm(h_prev[...], w_prev[low : low + inter, :]).astype(jnp.bfloat16).astype(jnp.float32)
                for j in range(inter // LANES):
                    for odd in (0, 1):
                        at = pl.ds((k * (inter // LANES) + j) * PITCH + odd, half, stride=2)
                        o_now[at, :] = out[odd * half : (odd + 1) * half, j * LANES : (j + 1) * LANES]
            elif kind == "S":
                side_work(done, done + k * GROUP)
                done += k * GROUP
            else:
                h_now[...] = (jax.nn.silu(sums["G"]) * sums["U"]).astype(jnp.bfloat16)
        side_work(done, TILE)

    first_list = pltpu.make_async_copy(tab_hbm.at[tile_at(0), 0], t_next[RING - 1], lsem.at[RING - 1, 0])
    first_list.start()
    for ahead in range(RING - 1):
        for copy in list_copies(ahead, ahead):
            copy.start()
    first_list.wait()
    for r in range(TILE):
        x_bufs[0][pl.ds(r, pieces, stride=PITCH), :] = u_vm[row_at(t_next[RING - 1][r]), :]

    rounds = (count + RING + 1) // RING
    acc_in.wait()

    @pl.loop(0, rounds)
    def _(i):
        for turn in range(RING):
            tile_step(RING * i + turn, turn)

    for ahead in range(RING - 1):
        for copy in list_copies(RING * rounds + ahead, ahead):
            copy.wait()

    if last:

        def store_rows(step):
            slot = lax.rem(step, STAGES)
            return pltpu.make_async_copy(stage.at[slot], o_hbm.at[pl.ds(step * TILE, TILE), :], ssem.at[slot])

        @pl.loop(0, blocks)
        def _(step):
            @pl.when(step >= STAGES)
            def _():
                store_rows(step - STAGES).wait()

            parts = [acc[pl.ds(step * TILE * pieces + j, TILE, stride=pieces), :].astype(jnp.bfloat16) for j in range(pieces)]
            stage[lax.rem(step, STAGES)] = jnp.concatenate(parts, axis=1)
            store_rows(step).start()

        for step in range(blocks - min(STAGES, blocks), blocks):
            store_rows(step).wait()
    else:
        acc_out = pltpu.make_async_copy(acc.at[pl.ds(0, tokens * pieces), :], o_hbm, asem)
        acc_out.start()
        acc_out.wait()


def moe_call(last, meta, table, ranks, gates, u_norm, total, weights):
    tokens, width = u_norm.shape
    pieces = width // LANES
    experts = sum(w.shape[0] for w in weights)
    wrows, inter = weights[0].shape[1:]
    smem = pl.BlockSpec(memory_space=pltpu.SMEM)
    hbm = pl.BlockSpec(memory_space=pl.ANY)
    scratch = [
        pltpu.VMEM((tokens * pieces + 8, LANES), jnp.float32),
        pltpu.VMEM((tokens * pieces + 8, LANES), jnp.float32),
        pltpu.VMEM((3, wrows, inter), jnp.bfloat16),
        *[pltpu.VMEM((pieces * PITCH, LANES), jnp.float32)] * 4,
        *[pltpu.VMEM((TILE, inter), jnp.bfloat16)] * 2,
        *[pltpu.SMEM((TILE,), jnp.int32)] * (3 * RING),
        pltpu.VMEM((STAGES, TILE, width), jnp.bfloat16),
        pltpu.SemaphoreType.DMA((3,)),
        pltpu.SemaphoreType.DMA((STAGES,)),
        pltpu.SemaphoreType.DMA,
        pltpu.SemaphoreType.DMA((RING, 3)),
    ]
    out_shape = jax.ShapeDtypeStruct((tokens, width), jnp.bfloat16) if last else jax.ShapeDtypeStruct((tokens * pieces, LANES), jnp.float32)
    rows = experts * tokens // 8
    return pl.pallas_call(
        functools.partial(moe_kernel, last, len(weights)),
        in_specs=[smem] * 3 + [hbm] * (3 + len(weights)),
        out_specs=hbm,
        out_shape=out_shape,
        scratch_shapes=scratch,
        compiler_params=pltpu.CompilerParams(vmem_limit_bytes=VMEM_LIMIT),
        cost_estimate=pl.CostEstimate(flops=2 * rows * wrows * inter, bytes_accessed=2 * experts * wrows * inter, transcendentals=0),
        name="routed_experts",
    )(meta, ranks, gates, table, u_norm, total, *weights)


def route_plan(choice_ids, num_experts, groups, here):
    tokens, num_top = choice_ids.shape
    local = num_experts // groups
    device, index = choice_ids // local, choice_ids % local
    rank = jnp.zeros_like(choice_ids)
    low = 0
    for way, size in PLAN:
        place = device ^ here if way == "P" else device
        rank = jnp.where((index >= low) & (index < low + size), low * groups + place * size + index - low, rank)
        low += size
    hits = rank[:, :, None] == jnp.arange(num_experts)[None, None, :]
    counts = jnp.sum(hits.astype(jnp.int32), axis=(0, 1))
    slots = jnp.arange(tokens)[:, None] * num_top + jnp.arange(num_top)[None, :]
    keys = (rank * 65536 + slots).reshape(-1)
    spare = jnp.arange(TILE)[None, :] < ((-counts) % TILE)[:, None]
    dummy = tokens * num_top
    fill = jnp.where(spare, jnp.arange(num_experts)[:, None] * 65536 + dummy, num_experts * 65536 + dummy)
    ordered = jnp.sort(jnp.concatenate([keys, fill.reshape(-1)]), stable=False)
    tiles = (counts + TILE - 1) // TILE
    spans = [(sum(CHUNKS[:i]) * groups, sum(CHUNKS[: i + 1]) * groups) for i in range(len(CHUNKS))]
    experts = jnp.arange(num_experts)
    chunk = sum((experts >= low).astype(jnp.int32) for low, _ in spans) - 1
    used = counts > 0
    ahead = (chunk[:, None] == chunk[None, :]) & (experts[None, :] < experts[:, None])
    order = jnp.sum(jnp.where(ahead & used[None, :], 1, 0), axis=1)
    start = jnp.array([low for low, _ in spans])
    stop = jnp.array([high for _, high in spans])
    member = (experts[None, :] >= start[:, None]) & (experts[None, :] < stop[:, None]) & used[None, :]
    names = jnp.sum(jnp.where(member[:, None, :] & (order[None, None, :] == experts[None, :, None]), experts[None, None, :] - start[:, None, None], 0), axis=2)
    first = jnp.sum(jnp.where(experts[None, :] < start[:, None], tiles[None, :], 0), axis=1)
    final = jnp.sum(jnp.where(experts[None, :] < stop[:, None], tiles[None, :], 0), axis=1)
    metas = jnp.concatenate([jnp.stack([first, final, jnp.sum(member.astype(jnp.int32), axis=1)], axis=1), names], axis=1).astype(jnp.int32)
    ranks = ordered[::TILE] // 65536
    orders = jnp.sum(jnp.where(ranks[:, None] == experts[None, :], order[None, :], 0), axis=1)
    low = ordered & 65535
    table = jnp.stack([(low & ~7).reshape(-1, TILE), low.reshape(-1, TILE)], axis=1)
    return table, orders, metas


def after(vals, token):
    return lax.optimization_barrier((vals, token))[0]


def spread_pair(own, early, late):
    count = lax.axis_size(AXIS)

    def send(bit, vals):
        return lax.ppermute(vals, AXIS, [(i, i ^ bit) for i in range(count)])

    own = after(own, early)
    along_x, along_y = after((send(2, own), send(4, own)), late)
    far = send(4, along_x[:1]), send(2, along_y[1:])
    own_core = [own, along_x, along_y, *far]
    other = [send(1, vals) for vals in own_core]
    return (own, other[0], along_x, other[1], along_y, other[2], *far, *other[3:])


def solution(mesh):
    groups = mesh.shape[AXIS]
    rows_spec = P(AXIS, None)
    vec_spec = P(AXIS)
    full_spec = P(None, None)
    cube_spec = P(AXIS, None, None)
    in_specs = (cube_spec, vec_spec, rows_spec, rows_spec, rows_spec, vec_spec, rows_spec, vec_spec, rows_spec, rows_spec, vec_spec, rows_spec, rows_spec, rows_spec, vec_spec, full_spec, cube_spec, cube_spec, cube_spec, full_spec, full_spec, full_spec, cube_spec)

    def gather(shard):
        return lax.all_gather(shard, AXIS, axis=0, tiled=True)

    def local(x_resid, g_mlp, w_gate, w_up, w_down, g_attn, w_dq, g_q, w_uq, w_dkv, g_kv, w_uk, w_uv, w_out, g_moe, w_router, we_gate, we_up, we_down, ws_gate, ws_up, ws_down, expert_ids):
        num_seqs, seq_len, width = x_resid.shape
        tokens = num_seqs * seq_len
        num_experts = w_router.shape[0]
        inter = we_gate.shape[2]
        flat_x = x_resid.reshape(tokens, width)
        choice_ids = expert_ids.reshape(tokens, expert_ids.shape[2])

        gains = [g_mlp, g_attn, g_q, g_kv, g_moe]
        sizes = [g.shape[0] for g in gains]
        here = lax.axis_index(AXIS)
        vectors = jnp.concatenate(gains)[None]
        bit = 1
        while bit < groups:
            other = lax.ppermute(vectors, AXIS, [(i, i ^ bit) for i in range(groups)])
            mine_first = (here & bit) == 0
            vectors = jnp.where(mine_first, jnp.concatenate([vectors, other]), jnp.concatenate([other, vectors]))
            bit *= 2
        offs = [sum(sizes[:i]) for i in range(len(sizes))]
        g_mlp, g_attn, g_q, g_kv, g_moe = [vectors[:, o : o + s].reshape(-1) for o, s in zip(offs, sizes)]

        inner = w_gate.shape[1]
        dense_w = gather(jnp.concatenate([to_blocks(jnp.concatenate([w_gate, w_up], axis=1), DENSE_LANES), to_blocks(w_down, DENSE_LANES)])[None])
        dense_at = (0, 2 * inner // DENSE_LANES * w_gate.shape[0])
        kv_rank = w_uk.shape[0] * groups
        rope_dim = w_dkv.shape[1] - kv_rank
        nope = w_uk.shape[1]
        heads = (w_uq.shape[1] - nope) // rope_dim
        nope_dim = nope // heads
        per_head = w_uq.reshape(w_uq.shape[0], heads, nope_dim + rope_dim)
        uq_local = jnp.concatenate([per_head[:, :, :nope_dim].reshape(-1, nope), per_head[:, :, nope_dim:].reshape(-1, heads * rope_dim)], axis=1)
        shards = [jnp.concatenate([w_dq, w_dkv, w_dkv[:, kv_rank:]], axis=1), uq_local, w_uk, w_uv, w_out]
        blocks = [to_blocks(s, ATTN_LANES) for s in shards]
        attn_w = gather(jnp.concatenate(blocks, axis=0)[None])
        attn_at = tuple(sum(b.shape[0] for b in blocks[:i]) for i in range(len(blocks)))

        down_blocks = we_down.reshape(we_down.shape[0], inter, width // inter, inter).transpose(0, 2, 1, 3).reshape(we_down.shape[0], width, inter)
        pack = jnp.concatenate([we_gate, we_up, down_blocks], axis=1)
        table, ranks, metas = route_plan(choice_ids, num_experts, groups, lax.axis_index(AXIS))

        h_one = dense_layer(dense_w, dense_at, flat_x, g_mlp, inner)
        expert_w = []
        low = 0
        for way, size in PLAN:
            part = pack[low : low + size]
            expert_w.append(spread_pair(part, dense_w, h_one) if way == "P" else (gather(part),))
            low += size

        positions = jnp.arange(seq_len)
        inv_freq = 1.0 / (ROPE_BASE ** (jnp.arange(0, rope_dim, 2).astype(jnp.float32) / rope_dim))
        angles = positions.astype(jnp.float32)[:, None] * inv_freq[None, :]
        cos_t, sin_t = jnp.cos(angles), jnp.sin(angles)
        cos_w = jnp.concatenate([cos_t] * 4, axis=1)
        sin_w = jnp.concatenate([-sin_t, sin_t] * 2, axis=1)
        queries_keys = attention_prep(attn_w, attn_at[:4], h_one, g_attn, g_q, g_kv, cos_w, sin_w, nope, heads * rope_dim)
        attended = attention_core(*queries_keys, seq_len, (nope_dim + rope_dim) ** -0.5)

        terms, rest = [], w_router
        for _ in range(3):
            terms.append(lax.reduce_precision(rest, 8, 7))
            rest = rest - terms[-1]
        terms.append(jnp.zeros_like(rest))
        wr = jnp.concatenate(terms).astype(jnp.bfloat16)
        u_norm, scores, total = attention_post(attn_w, attn_at[4:], attended, h_one, g_moe, wr, jnp.concatenate([ws_gate, ws_up], axis=1), ws_down)
        scores = scores[:, :num_experts]
        hits = choice_ids[:, :, None] == jnp.arange(num_experts)[None, None, :]
        picked = jnp.sum(jnp.where(hits, scores[:, None, :], 0.0), axis=2)
        gates = (ROUTE_SCALE * picked / jnp.sum(picked, axis=1, keepdims=True)).reshape(-1)
        gates = jnp.concatenate([gates, jnp.zeros((8,), jnp.float32)])
        for i, weights in enumerate(expert_w):
            total = moe_call(i == len(expert_w) - 1, metas[i], table, ranks, gates, u_norm, total, weights)
        return total.reshape(num_seqs, seq_len, width)

    return jax.shard_map(local, mesh=mesh, in_specs=in_specs, out_specs=cube_spec, check_vma=False)
```
